32 devices in a mesh: task: 8 (over z, core), tp: 4 (over y, x).
Axes of the slice: x: 2, y: 2, z: 4, core: 2. Of those that a mesh axis runs over, the one named last changes fastest.
Arguments:
- support_x: bfloat16 [8, 384, 3584], P('task'), may hold values from -6 to 6
- adapter_a: bfloat16 [8, 3584, 64], P('task'), may hold values from -0.09375 to 0.09375
- gate_pre: bfloat16 [8, 384, 10240], P('task', None, 'tp'), may hold values from -6 to 6
- lengths: int32 [8], P('task'), may hold values from 128 to 384, as said below
- damping: float32 [8], P('task'), may hold values from 0.03 to 0.3
- down_w: bfloat16 [10240, 3584], P('tp', 'task'), may hold values from -0.0625 to 0.0625
- grad_b: float32 [8, 64, 10240], P('task', None, 'tp'), may hold values from -6 to 6
Outputs:
- solution: float32 [8, 64, 10240], P('task', None, 'tp')
- residual: float32 [8, 64, 10240], P('task', None, 'tp')
The draws below stay inside these ranges and needn't reach their ends.
Inputs may be any that keep to these rules, and one draw needn't show every extreme that they name: `lengths`: each a multiple of 128; some task has exactly 384.
All inputs are finite; a program needn't handle non-finite values.
Results may differ from the reference program's by a relative error of at most 0.033.
Values may be sent and summed in bfloat16 or wider, within the bound.
A program may use at most 64 MiB of HBM per device.

```python
import math
import jax
import jax.numpy as jnp
from jax import lax

D = 3584
FF_WIN = 10240
RANK = 64
BLOCK = 128
LEN = 384
ITERS = 2
TASKS = 8
N_TP = 4


def draw_lengths(key, part):
    blocks = jax.random.randint(key, (TASKS,), 1, LEN // BLOCK + 1)
    chosen = jax.random.randint(jax.random.fold_in(key, 7), (), 0, TASKS)
    blocks = jnp.where(jnp.arange(TASKS) == chosen, LEN // BLOCK, blocks)
    return (blocks * BLOCK).astype(jnp.int32)


def shard_levels(key, extent, split, low, top_value):
    loudness, own = 1.0, jax.random.fold_in(key, 6)
    for dim, shards_of in split:
        draws = jnp.exp(jax.random.uniform(jax.random.fold_in(own, dim), (shards_of,), jnp.float32, low / len(split), top_value / len(split)))
        loudness = loudness * jnp.repeat(draws, extent[dim] // shards_of).reshape([-1 if axis == dim else 1 for axis in range(len(extent))])
    return loudness


def gaussian(rng, shape, scale, reach, pieces=(), kind=jnp.bfloat16):
    values = scale * jax.random.normal(rng, shape, jnp.float32)
    if pieces:
        values = values * shard_levels(rng, shape, pieces, -0.22, 0.18)
    return jnp.clip(values, -reach, reach).astype(kind)


def setup_inputs(seed: int = 0) -> dict:
    streams_of = jax.random.split(jax.random.key(seed), 8)
    support_x = gaussian(streams_of[0], (TASKS, LEN, D), 1.0, 6.0, ((0, 8),))
    adapter_a = gaussian(streams_of[1], (TASKS, D, RANK), D ** -0.5, 0.09375, ((0, 8),))
    gate_pre = gaussian(streams_of[2], (TASKS, LEN, FF_WIN), 1.0, 6.0, ((0, 8), (2, 4)))
    lengths = draw_lengths(jax.random.fold_in(streams_of[7], 71), 0)
    damping = jnp.clip(jnp.exp(math.log(0.3) - 2.3025852 * jax.random.uniform(streams_of[4], (TASKS,), jnp.float32) ** shard_levels(streams_of[4], (TASKS,), ((0, 8),), -0.2, 0.2)), 0.03, 0.3)
    down_w = gaussian(streams_of[5], (FF_WIN, D), FF_WIN ** -0.5, 0.0625, ((0, 4), (1, 8)))
    grad_b = gaussian(streams_of[6], (TASKS, RANK, FF_WIN), 1.0, 6.0, ((0, 8), (2, 4)), jnp.float32)
    return dict(support_x=support_x, adapter_a=adapter_a, gate_pre=gate_pre, lengths=lengths, damping=damping, down_w=down_w, grad_b=grad_b)


def solve_task(operands, down_w):
    support, adapter, gate, length, damping_rate, target = operands
    width = FF_WIN // N_TP
    features = jnp.dot(support, adapter, preferred_element_type=jnp.float32).astype(jnp.bfloat16)
    positions = jnp.arange(LEN, dtype=jnp.int32)[:, None]
    gated = jnp.where(positions < length, jax.nn.silu(gate.astype(jnp.float32)), 0.0).astype(jnp.bfloat16)
    tokens_live = length.astype(jnp.float32)
    weights = down_w.reshape(N_TP, width, D).astype(jnp.float32)

    def apply(vector):
        inner = jnp.dot(features, vector.astype(jnp.bfloat16), preferred_element_type=jnp.float32)
        active = (gated.astype(jnp.float32) * inner).astype(jnp.bfloat16)
        grouped = active.reshape(LEN, N_TP, width).astype(jnp.float32)
        partial_sums = jnp.einsum("lgf,gfd->lgd", grouped, weights)
        rounded = lax.optimization_barrier(partial_sums.astype(jnp.bfloat16))
        mixed = jnp.sum(rounded.astype(jnp.float32), axis=1).astype(jnp.bfloat16)
        back = jnp.dot(mixed, down_w.T, preferred_element_type=jnp.float32)
        second = (gated.astype(jnp.float32) * back).astype(jnp.bfloat16)
        return jnp.dot(features.T, second, preferred_element_type=jnp.float32) / tokens_live + damping_rate * vector

    solution = jnp.zeros_like(target)
    residual = target
    direction = target
    norm_now = jnp.sum(residual * residual)
    for step in range(ITERS):
        image = apply(direction)
        alpha = norm_now / jnp.sum(direction * image)
        solution = solution + alpha * direction
        residual = residual - alpha * image
        norm_next = jnp.sum(residual * residual)
        direction = residual + (norm_next / norm_now) * direction
        norm_now = norm_next
    return solution, residual


def reference(support_x, adapter_a, gate_pre, lengths, damping, down_w, grad_b):
    def per_task(operands):
        return solve_task(operands, down_w)

    return lax.map(per_task, (support_x, adapter_a, gate_pre, lengths, damping, grad_b))
```

```python
import jax
import jax.numpy as jnp
from jax import lax
from jax.experimental import pallas as pl
from jax.experimental.pallas import tpu as pltpu
from jax.sharding import PartitionSpec as P

ITERS = 2


def shards(support_x, adapter_a, gate_pre, lengths, damping, down_w, grad_b):
    down_full = lax.all_gather(down_w, "task", axis=1, tiled=True)
    features = jnp.dot(support_x[0], adapter_a[0], preferred_element_type=jnp.float32).astype(
        jnp.bfloat16
    )
    positions = lax.broadcasted_iota(jnp.int32, (gate_pre.shape[1], 1), 0)
    gated = jnp.where(
        positions < lengths[0], jax.nn.silu(gate_pre[0].astype(jnp.float32)), 0.0
    ).astype(jnp.bfloat16)
    tokens_live = lengths[0].astype(jnp.float32)
    damping_rate = damping[0]

    def transposed(mixed_rows):
        return lax.dot_general(
            mixed_rows, down_full, (((1,), (1,)), ((), ())), preferred_element_type=jnp.float32
        )

    def apply(vector):
        inner = jnp.dot(features, vector.astype(jnp.bfloat16), preferred_element_type=jnp.float32)
        active = (gated * inner).astype(jnp.bfloat16)
        partial_sum = jnp.dot(active, down_full, preferred_element_type=jnp.float32)
        mixed = lax.psum(partial_sum.astype(jnp.bfloat16), "tp")
        second = (gated * transposed(mixed)).astype(jnp.bfloat16)
        product = lax.dot_general(
            features, second, (((0,), (0,)), ((), ())), preferred_element_type=jnp.float32
        )
        return product / tokens_live + damping_rate * vector

    def paired_sums(vector, image):
        return lax.psum((jnp.sum(vector * vector), jnp.sum(vector * image)), "tp")

    target = grad_b[0]
    solution = jnp.zeros_like(target)
    residual = target
    image = apply(residual)
    norm_now, product = paired_sums(residual, image)
    alpha = norm_now / product
    direction, along = (residual, image)
    for step in range(ITERS):
        solution = solution + alpha * direction
        residual = residual - alpha * along
        if step + 1 < ITERS:
            image = apply(residual)
            norm_next, product = paired_sums(residual, image)
            ratio = norm_next / norm_now
            alpha = norm_next / (product - ratio * norm_next / alpha)
            direction = residual + ratio * direction
            along = image + ratio * along
            norm_now = norm_next
    return (solution[None], residual[None])


MESH = pl.DeviceIdType.MESH
HALF = 64
UNIT = 2 * HALF
CHUNK = 256
AHEAD = 3
EARLY = 3


def arrival_order(subs):
    near, far = list(range(subs)), list(range(subs - 1, -1, -1))
    gate = subs
    clock, times = 0.0, []
    for place in near:
        if place == AHEAD:
            clock += gate
        clock += 1.0
        times.append((clock, place))
    events = [(when, 0, place) for when, place in times]
    events += [(place + 1.0, 1, 2 * subs + far[place]) for place in near]
    clock = float(subs)
    for when, place in times:
        clock = max(clock, when) + 1.0
        events.append((clock, 2, 3 * subs + far[place]))
    middle = [subs + place for place in near] + [unit for _, _, unit in sorted(events)]
    end = near + [subs + place for place in near] + [2 * subs + place for place in far]
    return end + [0] * subs, middle


def kernel(
    support_hbm, adapter_hbm, gate_hbm, length_ref, damping_ref, w_hbm, grad_hbm,
    sol_ref, res_ref,
    support, adapter, grad, weights, gated, active, total, features, image0, image1,
    far_gated, far_active, far_total, far_features, vector16, far_vector, far_image, image_got,
    part1, got1, mixed1, part2, pass2, added2, got2, mixed2, sums, sums_got,
    load_sem, w_recv, p_recv, in_send, out_send, d2d_send, far_send, far_recv,
    rs_send1, rs_recv1, ag_send1, ag_recv1, rs_send2, pass_recv2, rs_recv2,
    ag_send2, ag_recv2, fw_send, fw_recv, sum_send, sum_recv,
):
    t_me, j_me = lax.axis_index("task"), lax.axis_index("tp")
    z, core = t_me // 2, t_me % 2
    other = 1 - core
    upper = z // 2
    inner = z + upper * (3 - 2 * z)
    n_tp, rows = part1.shape[1:3]
    tokens, hidden = active.shape
    width = weights.shape[0]
    subs = w_hbm.shape[0] // HALF
    n_unit = 4 * subs
    n_chunk = part2.shape[0]
    tile = far_image.shape[2]
    n_tile = hidden // tile
    orders = arrival_order(subs)

    def unit_of(e):
        unit = orders[0][0] + inner * (orders[1][0] - orders[0][0])
        for place in range(1, n_unit):
            first, second = orders[0][place], orders[1][place]
            unit = jnp.where(e == place, first + inner * (second - first), unit)
        return unit

    def placed(p):
        return p + upper * (n_unit - 1 - 2 * p)

    def half(p, side):
        return weights.at[pl.ds(pl.multiple_of(placed(p) * UNIT + side * HALF, HALF), HALF)]

    def span(p):
        return pl.ds(pl.multiple_of(placed(p) * UNIT, UNIT), UNIT)

    own = [
        pltpu.make_async_copy(
            w_hbm.at[pl.ds(s * HALF, HALF)],
            weights.at[pl.ds(pl.multiple_of((z * subs + s) * UNIT + core * HALF, HALF), HALF)],
            load_sem.at[0],
        )
        for s in range(subs)
    ]
    for load in own:
        load.start()
    loads = [
        pltpu.make_async_copy(source, target, load_sem.at[1 + place])
        for place, (source, target) in enumerate(
            ((gate_hbm, active), (support_hbm, support), (adapter_hbm, adapter), (grad_hbm, grad))
        )
    ]
    for load in loads:
        load.start()

    inward = {"task": t_me + 2 - 4 * upper, "tp": j_me}
    outward = {"task": t_me - 2 + 4 * upper, "tp": j_me}
    partner = {"task": 2 * z + other, "tp": j_me}
    peers = [{"task": t_me, "tp": lax.rem(j_me + d, n_tp)} for d in range(1, n_tp)]

    barrier = pltpu.get_barrier_semaphore()
    for peer in [partner, inward] + peers:
        pl.semaphore_signal(barrier, inc=1, device_id=peer, device_id_type=MESH)

    @pl.when(inner == 1)
    def _():
        pl.semaphore_signal(barrier, inc=1, device_id=outward, device_id_type=MESH)

    pl.semaphore_wait(barrier, n_tp + 1 + inner)

    def drained(ref, sem):
        pltpu.make_async_copy(ref, ref, sem).wait()

    def push(src, dst, send_sem, recv_sem, target):
        pltpu.make_async_remote_copy(
            src_ref=src, dst_ref=dst, send_sem=send_sem, recv_sem=recv_sem,
            device_id=target, device_id_type=MESH,
        ).start()

    def send_half(p, target, send_sem):
        push(half(p, core), half(p, core), send_sem.at[0], w_recv.at[placed(p)], target)

    def share_half(p):
        push(half(p, core), half(p, core), d2d_send.at[0], p_recv.at[placed(p)], partner)

    def arrive(p):
        drained(half(p, core), w_recv.at[placed(p)])

        @pl.when((inner == 1) & (p < subs))
        def _():
            send_half(p, inward, in_send)

        @pl.when((inner == 1) & (p >= 2 * subs) & ((p < 3 * subs) | (p >= n_unit - EARLY)))
        def _():
            send_half(p, outward, out_send)

        share_half(p)

    def completed(p):
        drained(half(p, other), p_recv.at[placed(p)])

    first = inner * subs
    drained(weights.at[pl.ds(0, subs * HALF)], load_sem.at[0])

    @pl.loop(0, AHEAD)
    def _(s):
        send_half(first + s, inward, in_send)

        @pl.when(inner == 1)
        def _():
            send_half(first + s, outward, out_send)

        share_half(first + s)

    @pl.when(inner == 1)
    def _():
        @pl.loop(AHEAD, subs)
        def _(s):
            send_half(first + s, inward, in_send)
            send_half(first + s, outward, out_send)

    @pl.loop(AHEAD, subs)
    def _(s):
        share_half(first + s)

    loads[1].wait()
    loads[2].wait()
    features[...] = lax.dot_general(
        support[...], adapter[...], (((1,), (1,)), ((), ())), preferred_element_type=jnp.float32
    ).astype(jnp.bfloat16)
    loads[0].wait()
    loads[3].wait()
    live, rate = length_ref[0].astype(jnp.float32), damping_ref[0]
    positions = lax.broadcasted_iota(jnp.int32, (tokens, tile), 0).astype(jnp.float32)

    def columns(i):
        return pl.ds(pl.multiple_of(i * tile, tile), tile)

    @pl.loop(0, n_tile)
    def _(i):
        pre = active[:, columns(i)].astype(jnp.float32)
        gated[:, columns(i)] = jnp.where(
            positions < live, pre / (1.0 + jnp.exp(-pre)), 0.0
        ).astype(jnp.bfloat16)
        vector16[:, columns(i)] = grad[:, columns(i)].astype(jnp.bfloat16)

    @pl.when(inner == 0)
    def _():
        for place, (src, dst) in enumerate(
            ((features, far_features), (vector16, far_vector), (gated, far_gated))
        ):
            push(src, dst, far_send.at[place], far_recv.at[place], inward)

        @pl.loop(AHEAD, subs)
        def _(s):
            send_half(first + s, inward, in_send)

    @pl.when(inner == 1)
    def _():
        image_got[...] = jnp.zeros_like(image_got)

    def make_active(feats, vector, gate, act, tot):
        @pl.loop(0, n_tile)
        def _(i):
            wide = jnp.dot(
                feats[...], vector[:, columns(i)], preferred_element_type=jnp.float32
            )
            act[:, columns(i)] = (gate[:, columns(i)].astype(jnp.float32) * wide).astype(
                jnp.bfloat16
            )
            tot[:, columns(i)] = jnp.zeros_like(wide)

    def product(slot, p, act):
        partial_sum = lax.dot_general(
            act[...], weights[span(p), :], (((1,), (1,)), ((), ())),
            preferred_element_type=jnp.float32,
        )
        part1[slot] = partial_sum.astype(jnp.bfloat16).reshape(n_tp, rows, UNIT)
        for d in range(1, n_tp):
            push(
                part1.at[slot, lax.rem(j_me + d, n_tp)], got1.at[slot, d - 1],
                rs_send1.at[0], rs_recv1.at[slot], peers[d - 1],
            )

    def reduce(slot):
        drained(got1.at[slot], rs_recv1.at[slot])
        added = part1[slot, j_me].astype(jnp.float32)
        for d in range(1, n_tp):
            added = added + got1[slot, d - 1].astype(jnp.float32)
        mixed1[slot, j_me] = added.astype(jnp.bfloat16)
        for peer in peers:
            push(
                mixed1.at[slot, j_me], mixed1.at[slot, j_me],
                ag_send1.at[0], ag_recv1.at[slot], peer,
            )

    def back(slot, p, tot):
        drained(mixed1.at[slot, pl.ds(0, n_tp - 1)], ag_recv1.at[slot])
        whole = mixed1[slot].reshape(tokens, UNIT)

        @pl.loop(0, n_tile)
        def _(i):
            tot[:, columns(i)] += jnp.dot(
                whole, weights[span(p), columns(i)], preferred_element_type=jnp.float32
            )

    def make_image(vector, image, slot, extra):
        def body(i, carry):
            second = (gated[:, columns(i)].astype(jnp.float32) * total[:, columns(i)]).astype(
                jnp.bfloat16
            )
            outer = lax.dot_general(
                features[...], second, (((0,), (0,)), ((), ())),
                preferred_element_type=jnp.float32,
            )
            if extra is not None:
                outer = outer + extra[i].astype(jnp.float32)
            v = vector[:, columns(i)]
            value = outer / live + rate * v
            image[:, columns(i)] = value
            return carry[0] + v * v, carry[1] + v * value

        zero = jnp.zeros((vector.shape[0], tile), jnp.float32)
        squares, crosses = lax.fori_loop(0, n_tile, body, (zero, zero))
        sums[slot, 0] = jnp.broadcast_to(jnp.sum(squares, keepdims=True), (8, 128))
        sums[slot, 1] = jnp.broadcast_to(jnp.sum(crosses, keepdims=True), (8, 128))
        for d in range(1, n_tp):
            push(
                sums.at[slot], sums_got.at[slot, d - 1],
                sum_send.at[slot], sum_recv.at[slot], peers[d - 1],
            )
        drained(sums_got.at[slot], sum_recv.at[slot])
        norm, cross = sums[slot, 0, 0:1, 0:1], sums[slot, 1, 0:1, 0:1]
        for d in range(1, n_tp):
            norm = norm + sums_got[slot, d - 1, 0, 0:1, 0:1]
            cross = cross + sums_got[slot, d - 1, 1, 0:1, 0:1]
        return norm, cross

    make_active(features, vector16, gated, active, total)
    count = n_unit - subs + inner * subs

    @pl.loop(0, count + 2)
    def _(e):
        p, before, earlier = unit_of(e), unit_of(e - 1), unit_of(e - 2)

        @pl.when((e >= 1) & (e <= count))
        def _():
            reduce(e - 1)

            @pl.when(before >= 3 * subs)
            def _():
                reduce(before + subs)

        @pl.when(e >= 2)
        def _():
            @pl.when(earlier >= 3 * subs)
            def _():
                back(earlier + subs, earlier, far_total)

            back(e - 2, earlier, total)

        @pl.when(e < count)
        def _():
            @pl.when(e >= subs)
            def _():
                arrive(p)

            completed(p)

            @pl.when(p >= 3 * subs)
            def _():
                @pl.when(p == n_unit - 1)
                def _():
                    for place, ref in enumerate((far_features, far_vector, far_gated)):
                        drained(ref, far_recv.at[place])
                    make_active(far_features, far_vector, far_gated, far_active, far_total)

                product(p + subs, p, far_active)

            product(e, p, active)

    @pl.when(inner == 1)
    def _():
        @pl.loop(0, n_tile)
        def _(i):
            second = (
                far_gated[:, columns(i)].astype(jnp.float32) * far_total[:, columns(i)]
            ).astype(jnp.bfloat16)
            far_image[i] = lax.dot_general(
                far_features[...], second, (((0,), (0,)), ((), ())),
                preferred_element_type=jnp.float32,
            ).astype(jnp.bfloat16)
            push(far_image.at[i], image_got.at[i], far_send.at[3], far_recv.at[3], outward)

        @pl.loop(0, subs - EARLY)
        def _(s):
            send_half(n_unit - 1 - EARLY - s, outward, out_send)

    @pl.when(inner == 0)
    def _():
        @pl.loop(0, EARLY)
        def _(s):
            arrive(n_unit - 1 - s)

        drained(image_got, far_recv.at[3])

    norm0, cross0 = make_image(grad, image0, 0, image_got)
    alpha0 = norm0 / cross0

    @pl.loop(0, n_tile)
    def _(i):
        value = grad[:, columns(i)] - alpha0 * image0[:, columns(i)]
        res_ref[:, columns(i)] = value
        wide = jnp.dot(
            features[...], value.astype(jnp.bfloat16), preferred_element_type=jnp.float32
        )
        active[:, columns(i)] = (gated[:, columns(i)].astype(jnp.float32) * wide).astype(
            jnp.bfloat16
        )
        total[:, columns(i)] = jnp.zeros_like(wide)

    row, col = j_me // 2, j_me % 2
    beside, below = 2 * row + 1 - col, 2 * (1 - row) + col
    across = n_tp - 1 - j_me
    top, low = pl.ds(0, rows // 2), pl.ds(rows // 2, rows // 2)
    side, under = {"task": t_me, "tp": beside}, {"task": t_me, "tp": below}
    early = 3 * subs * UNIT // CHUNK

    def stretch(i):
        c = jnp.where(i < early, i, n_chunk - 1 + early - i)
        start = c * CHUNK + upper * (width - CHUNK - 2 * c * CHUNK)
        return c, pl.ds(pl.multiple_of(start, CHUNK), CHUNK)

    def product2(i):
        c, where = stretch(i)

        @pl.when((inner == 0) & (i >= early))
        def _():
            for p in (2 * c + 1, 2 * c):
                @pl.when(p >= 3 * subs)
                def _(p=p):
                    @pl.when(p < n_unit - EARLY)
                    def _():
                        arrive(p)

                    completed(p)

        partial_sum = lax.dot_general(
            active[...], weights[where, :], (((1,), (1,)), ((), ())),
            preferred_element_type=jnp.float32,
        )
        part2[i] = partial_sum.astype(jnp.bfloat16).reshape(n_tp, rows, CHUNK)
        push(part2.at[i, across, top], pass2.at[i, 0], rs_send2.at[0], pass_recv2.at[i], side)
        push(part2.at[i, across, low], pass2.at[i, 1], rs_send2.at[0], pass_recv2.at[i], under)
        push(part2.at[i, beside, top], got2.at[i, 0, 0], rs_send2.at[0], rs_recv2.at[i], side)
        push(part2.at[i, below, low], got2.at[i, 1, 1], rs_send2.at[0], rs_recv2.at[i], under)

    def relay(i):
        drained(pass2.at[i], pass_recv2.at[i])
        for place, piece, where, target in ((0, below, top, under), (1, beside, low, side)):
            added2[i, place] = (
                part2[i, piece, where].astype(jnp.float32) + pass2[i, place].astype(jnp.float32)
            ).astype(jnp.bfloat16)
            push(
                added2.at[i, place], got2.at[i, 1 - place, place],
                rs_send2.at[0], rs_recv2.at[i], target,
            )

    def reduce2(i):
        drained(got2.at[i], rs_recv2.at[i])
        for place, where in ((0, top), (1, low)):
            mixed2[i, j_me, where] = (
                part2[i, j_me, where].astype(jnp.float32)
                + got2[i, 0, place].astype(jnp.float32)
                + got2[i, 1, place].astype(jnp.float32)
            ).astype(jnp.bfloat16)
        for target in (side, under):
            push(
                mixed2.at[i, j_me], mixed2.at[i, j_me],
                ag_send2.at[0], ag_recv2.at[i], target,
            )

    def forward2(i):
        drained(mixed2.at[i, pl.ds(0, 2)], ag_recv2.at[i])
        for source, where, target in ((beside, top, under), (below, low, side)):
            piece = mixed2.at[i, source, where]
            push(piece, piece, fw_send.at[0], fw_recv.at[i], target)

    def back2(i):
        _, where = stretch(i)
        drained(mixed2.at[i, 0], fw_recv.at[i])
        whole = mixed2[i].reshape(tokens, CHUNK)

        @pl.loop(0, n_tile)
        def _(k):
            total[:, columns(k)] += jnp.dot(
                whole, weights[where, columns(k)], preferred_element_type=jnp.float32
            )

    for start, stop in ((0, early), (early, n_chunk)):
        @pl.loop(start, stop)
        def _(i):
            product2(i)

        @pl.loop(start, stop)
        def _(i):
            relay(i)

        @pl.loop(start, stop)
        def _(i):
            reduce2(i)

    @pl.loop(0, n_chunk + 2)
    def _(i):
        @pl.when(i < n_chunk)
        def _():
            forward2(i)

        @pl.when(i >= 2)
        def _():
            back2(i - 2)

    norm1, cross1 = make_image(res_ref, image1, 1, None)
    ratio = norm1 / norm0
    alpha1 = norm1 / (cross1 - ratio * norm1 / alpha0)

    @pl.loop(0, n_tile)
    def _(i):
        first, then = grad[:, columns(i)], res_ref[:, columns(i)]
        sol_ref[:, columns(i)] = alpha0 * first + alpha1 * (then + ratio * first)
        res_ref[:, columns(i)] = then - alpha1 * (
            image1[:, columns(i)] + ratio * image0[:, columns(i)]
        )

    drained(weights.at[pl.ds(0, n_unit * HALF)], d2d_send.at[0])
    slots = part1.shape[0]

    @pl.when(inner == 0)
    def _():
        drained(weights.at[pl.ds(0, subs * HALF)], in_send.at[0])
        for place, ref in enumerate((features, vector16, gated)):
            drained(ref, far_send.at[place])
        for sem in (rs_send1, ag_send1):
            drained(got1.at[pl.ds(0, n_unit - subs)], sem.at[0])

    @pl.when(inner == 1)
    def _():
        drained(weights.at[pl.ds(0, 2 * subs * HALF)], in_send.at[0])
        drained(weights.at[pl.ds(0, 3 * subs * HALF)], out_send.at[0])
        drained(far_image, far_send.at[3])
        for sem in (rs_send1, ag_send1):
            drained(got1.at[pl.ds(0, slots)], sem.at[0])

    every = pl.ds(0, n_chunk)
    drained(mixed2.at[every, pl.ds(0, 3)], rs_send2.at[0])
    drained(mixed2.at[every, pl.ds(0, 2)], ag_send2.at[0])
    drained(mixed2.at[every, 0], fw_send.at[0])
    for slot in range(2):
        drained(sums_got.at[slot], sum_send.at[slot])


def fused(n_tp, support_x, adapter_a, gate_pre, lengths, damping, down_w, grad_b):
    tokens, width = support_x.shape[1:]
    rank = adapter_a.shape[2]
    hidden, share = down_w.shape
    subs = share // HALF
    n_unit = 4 * subs
    slots = n_unit + subs
    rows = tokens // n_tp
    n_chunk = width // CHUNK
    tile = next(size for size in (512, 256, 128) if hidden % size == 0)
    f32, bf16 = jnp.float32, jnp.bfloat16
    dma = pltpu.SemaphoreType.DMA
    anywhere, vmem = pl.BlockSpec(memory_space=pl.ANY), pl.BlockSpec(memory_space=pltpu.VMEM)
    smem = pl.BlockSpec(memory_space=pltpu.SMEM)
    shape = jax.ShapeDtypeStruct((rank, hidden), f32)
    solved, residual = pl.pallas_call(
        kernel,
        out_shape=(shape, shape),
        in_specs=[anywhere, anywhere, anywhere, smem, smem, anywhere, anywhere],
        out_specs=(vmem, vmem),
        scratch_shapes=[
            pltpu.VMEM((tokens, width), bf16),
            pltpu.VMEM((rank, width), bf16),
            pltpu.VMEM((rank, hidden), f32),
            pltpu.VMEM((width, hidden), bf16),
            pltpu.VMEM((tokens, hidden), bf16),
            pltpu.VMEM((tokens, hidden), bf16),
            pltpu.VMEM((tokens, hidden), f32),
            pltpu.VMEM((tokens, rank), bf16),
            pltpu.VMEM((rank, hidden), f32),
            pltpu.VMEM((rank, hidden), f32),
            pltpu.VMEM((tokens, hidden), bf16),
            pltpu.VMEM((tokens, hidden), bf16),
            pltpu.VMEM((tokens, hidden), f32),
            pltpu.VMEM((tokens, rank), bf16),
            pltpu.VMEM((rank, hidden), bf16),
            pltpu.VMEM((rank, hidden), bf16),
            pltpu.VMEM((hidden // tile, rank, tile), bf16),
            pltpu.VMEM((hidden // tile, rank, tile), bf16),
            pltpu.VMEM((slots, n_tp, rows, UNIT), bf16),
            pltpu.VMEM((slots, n_tp - 1, rows, UNIT), bf16),
            pltpu.VMEM((slots, n_tp, rows, UNIT), bf16),
            pltpu.VMEM((n_chunk, n_tp, rows, CHUNK), bf16),
            pltpu.VMEM((n_chunk, 2, rows // 2, CHUNK), bf16),
            pltpu.VMEM((n_chunk, 2, rows // 2, CHUNK), bf16),
            pltpu.VMEM((n_chunk, 2, 2, rows // 2, CHUNK), bf16),
            pltpu.VMEM((n_chunk, n_tp, rows, CHUNK), bf16),
            pltpu.VMEM((2, 2, 8, 128), f32),
            pltpu.VMEM((2, n_tp - 1, 2, 8, 128), f32),
            dma((5,)),
            dma((n_unit,)),
            dma((n_unit,)),
            dma((1,)),
            dma((1,)),
            dma((1,)),
            dma((4,)),
            dma((4,)),
            dma((1,)),
            dma((slots,)),
            dma((1,)),
            dma((slots,)),
            dma((1,)),
            dma((n_chunk,)),
            dma((n_chunk,)),
            dma((1,)),
            dma((n_chunk,)),
            dma((1,)),
            dma((n_chunk,)),
            dma((2,)),
            dma((2,)),
        ],
        compiler_params=pltpu.CompilerParams(
            collective_id=0, has_side_effects=True, vmem_limit_bytes=66_000_000
        ),
    )(
        support_x[0], adapter_a[0].T, gate_pre[0], lengths, damping, down_w.T, grad_b[0]
    )
    return solved[None], residual[None]


def solution(mesh):
    in_specs = (
        P("task", None, None),
        P("task", None, None),
        P("task", None, "tp"),
        P("task"),
        P("task"),
        P("tp", "task"),
        P("task", None, "tp"),
    )
    out_specs = (P("task", None, "tp"), P("task", None, "tp"))
    n_task, n_tp = mesh.shape["task"], mesh.shape["tp"]

    def body(support_x, *rest):
        tokens, width = support_x.shape[1:]
        hidden, share = rest[4].shape
        even = tokens % (32 * n_tp) == 0 and hidden % 128 == 0
        if n_tp != 4 or n_task != 8 or share % HALF or width % CHUNK or not even:
            return shards(support_x, *rest)
        return fused(n_tp, support_x, *rest)

    return jax.shard_map(body, mesh=mesh, in_specs=in_specs, out_specs=out_specs, check_vma=False)
```

```python
import jax
import jax.numpy as jnp
from jax import lax
from jax.experimental import pallas as pl
from jax.experimental.pallas import tpu as pltpu
from jax.sharding import PartitionSpec as P

ITERS = 2


def shards(support_x, adapter_a, gate_pre, lengths, damping, down_w, grad_b):
    down_full = lax.all_gather(down_w, "task", axis=1, tiled=True)
    features = jnp.dot(support_x[0], adapter_a[0], preferred_element_type=jnp.float32).astype(
        jnp.bfloat16
    )
    positions = lax.broadcasted_iota(jnp.int32, (gate_pre.shape[1], 1), 0)
    gated = jnp.where(
        positions < lengths[0], jax.nn.silu(gate_pre[0].astype(jnp.float32)), 0.0
    ).astype(jnp.bfloat16)
    tokens_live = lengths[0].astype(jnp.float32)
    damping_rate = damping[0]

    def transposed(mixed_rows):
        return lax.dot_general(
            mixed_rows, down_full, (((1,), (1,)), ((), ())), preferred_element_type=jnp.float32
        )

    def apply(vector):
        inner = jnp.dot(features, vector.astype(jnp.bfloat16), preferred_element_type=jnp.float32)
        active = (gated * inner).astype(jnp.bfloat16)
        partial_sum = jnp.dot(active, down_full, preferred_element_type=jnp.float32)
        mixed = lax.psum(partial_sum.astype(jnp.bfloat16), "tp")
        second = (gated * transposed(mixed)).astype(jnp.bfloat16)
        product = lax.dot_general(
            features, second, (((0,), (0,)), ((), ())), preferred_element_type=jnp.float32
        )
        return product / tokens_live + damping_rate * vector

    def paired_sums(vector, image):
        return lax.psum((jnp.sum(vector * vector), jnp.sum(vector * image)), "tp")

    target = grad_b[0]
    solution = jnp.zeros_like(target)
    residual = target
    image = apply(residual)
    norm_now, product = paired_sums(residual, image)
    alpha = norm_now / product
    direction, along = (residual, image)
    for step in range(ITERS):
        solution = solution + alpha * direction
        residual = residual - alpha * along
        if step + 1 < ITERS:
            image = apply(residual)
            norm_next, product = paired_sums(residual, image)
            ratio = norm_next / norm_now
            alpha = norm_next / (product - ratio * norm_next / alpha)
            direction = residual + ratio * direction
            along = image + ratio * along
            norm_now = norm_next
    return (solution[None], residual[None])


MESH = pl.DeviceIdType.MESH
HALF = 64
UNIT = 2 * HALF
CHUNK = 256
AHEAD = 2
EARLY = 3
LAG = 3


def arrival_order(subs):
    near, far = list(range(subs)), list(range(subs - 1, -1, -1))
    gate = subs
    clock, times = 0.0, []
    for place in near:
        if place == AHEAD:
            clock += gate
        clock += 1.0
        times.append((clock, place))
    events = [(when, 0, place) for when, place in times]
    events += [(place + 1.0, 1, 2 * subs + far[place]) for place in near]
    clock = float(subs)
    for when, place in times:
        clock = max(clock, when) + 1.0
        events.append((clock, 2, 3 * subs + far[place]))
    middle = [subs + place for place in near] + [unit for _, _, unit in sorted(events)]
    end = near + [subs + place for place in near] + [2 * subs + place for place in far]
    return end + [0] * subs, middle


def kernel(
    support_hbm, adapter_hbm, gate_hbm, length_ref, damping_ref, w_hbm, grad_hbm,
    sol_ref, res_ref,
    adapter, grad, weights, gated, active, total, features, image0, image1,
    far_gated, far_active, far_total, far_features, vector16, far_vector, far_image, image_got,
    part1, got1, mixed1, part2, pass2, added2, got2, mixed2, sums, sums_got,
    load_sem, w_recv, p_recv, in_send, out_send, d2d_send, far_send, far_recv,
    rs_send1, rs_recv1, ag_send1, ag_recv1, rs_send2, pass_recv2, rs_recv2,
    ag_send2, ag_recv2, fw_send, fw_recv, sum_send, sum_recv,
):
    t_me, j_me = lax.axis_index("task"), lax.axis_index("tp")
    z, core = t_me // 2, t_me % 2
    other = 1 - core
    upper = z // 2
    inner = z + upper * (3 - 2 * z)
    n_tp, rows = part1.shape[1:3]
    tokens, hidden = active.shape
    width = weights.shape[0]
    subs = w_hbm.shape[0] // HALF
    n_unit = 4 * subs
    n_chunk = part2.shape[0]
    tile = far_image.shape[2]
    n_tile = hidden // tile
    orders = arrival_order(subs)

    def unit_of(e):
        unit = orders[0][0] + inner * (orders[1][0] - orders[0][0])
        for place in range(1, n_unit):
            first, second = orders[0][place], orders[1][place]
            unit = jnp.where(e == place, first + inner * (second - first), unit)
        return unit

    def placed(p):
        return p + upper * (n_unit - 1 - 2 * p)

    def half(p, side):
        return weights.at[pl.ds(pl.multiple_of(placed(p) * UNIT + side * HALF, HALF), HALF)]

    def span(p):
        return pl.ds(pl.multiple_of(placed(p) * UNIT, UNIT), UNIT)

    own = [
        pltpu.make_async_copy(
            w_hbm.at[pl.ds(s * HALF, HALF)],
            weights.at[pl.ds(pl.multiple_of((z * subs + s) * UNIT + core * HALF, HALF), HALF)],
            load_sem.at[0],
        )
        for s in range(subs)
    ]
    for load in own:
        load.start()
    loads = [
        pltpu.make_async_copy(source, target, load_sem.at[1 + place])
        for place, (source, target) in enumerate(
            ((gate_hbm, active), (adapter_hbm, adapter), (grad_hbm, grad))
        )
    ] + [
        pltpu.make_async_copy(
            support_hbm.at[:, pl.ds(c * CHUNK, CHUNK)], part2.at[c], load_sem.at[4]
        )
        for c in range(n_chunk)
    ]
    for load in loads:
        load.start()

    inward = {"task": t_me + 2 - 4 * upper, "tp": j_me}
    outward = {"task": t_me - 2 + 4 * upper, "tp": j_me}
    partner = {"task": 2 * z + other, "tp": j_me}
    peers = [{"task": t_me, "tp": lax.rem(j_me + d, n_tp)} for d in range(1, n_tp)]

    barrier = pltpu.get_barrier_semaphore()
    for peer in [partner, inward] + peers:
        pl.semaphore_signal(barrier, inc=1, device_id=peer, device_id_type=MESH)

    @pl.when(inner == 1)
    def _():
        pl.semaphore_signal(barrier, inc=1, device_id=outward, device_id_type=MESH)

    pl.semaphore_wait(barrier, n_tp + 1 + inner)

    def drained(ref, sem):
        pltpu.make_async_copy(ref, ref, sem).wait()

    def push(src, dst, send_sem, recv_sem, target):
        pltpu.make_async_remote_copy(
            src_ref=src, dst_ref=dst, send_sem=send_sem, recv_sem=recv_sem,
            device_id=target, device_id_type=MESH,
        ).start()

    def send_half(p, target, send_sem):
        push(half(p, core), half(p, core), send_sem.at[0], w_recv.at[placed(p)], target)

    def share_half(p):
        push(half(p, core), half(p, core), d2d_send.at[0], p_recv.at[placed(p)], partner)

    def arrive(p):
        drained(half(p, core), w_recv.at[placed(p)])

        @pl.when((inner == 1) & (p < subs))
        def _():
            send_half(p, inward, in_send)

        @pl.when((inner == 1) & (p >= 2 * subs) & ((p < 3 * subs) | (p >= n_unit - EARLY)))
        def _():
            send_half(p, outward, out_send)

        share_half(p)

    def completed(p):
        drained(half(p, other), p_recv.at[placed(p)])

    first = inner * subs
    drained(weights.at[pl.ds(0, subs * HALF)], load_sem.at[0])

    @pl.loop(0, AHEAD)
    def _(s):
        send_half(first + s, inward, in_send)

        @pl.when(inner == 1)
        def _():
            send_half(first + s, outward, out_send)

        share_half(first + s)

    @pl.when(inner == 1)
    def _():
        @pl.loop(AHEAD, subs)
        def _(s):
            send_half(first + s, inward, in_send)
            send_half(first + s, outward, out_send)

    @pl.loop(AHEAD, subs)
    def _(s):
        share_half(first + s)

    loads[1].wait()
    drained(part2, load_sem.at[4])
    wide = jnp.zeros(features.shape, jnp.float32)
    for c in range(n_chunk):
        wide = wide + lax.dot_general(
            part2[c], adapter[:, pl.ds(c * CHUNK, CHUNK)], (((1,), (1,)), ((), ())),
            preferred_element_type=jnp.float32,
        )
    features[...] = wide.astype(jnp.bfloat16)
    loads[0].wait()
    loads[2].wait()
    live, rate = length_ref[0].astype(jnp.float32), damping_ref[0]
    positions = lax.broadcasted_iota(jnp.int32, (tokens, tile), 0).astype(jnp.float32)

    def columns(i):
        return pl.ds(pl.multiple_of(i * tile, tile), tile)

    @pl.loop(0, n_tile)
    def _(i):
        pre = active[:, columns(i)].astype(jnp.float32)
        gated[:, columns(i)] = jnp.where(
            positions < live, pre / (1.0 + jnp.exp(-pre)), 0.0
        ).astype(jnp.bfloat16)
        vector16[:, columns(i)] = grad[:, columns(i)].astype(jnp.bfloat16)

    @pl.when(inner == 0)
    def _():
        for place, (src, dst) in enumerate(
            ((features, far_features), (vector16, far_vector), (gated, far_gated))
        ):
            push(src, dst, far_send.at[place], far_recv.at[place], inward)

        @pl.loop(AHEAD, subs)
        def _(s):
            send_half(first + s, inward, in_send)

    @pl.when(inner == 1)
    def _():
        image_got[...] = jnp.zeros_like(image_got)

    def make_active(feats, vector, gate, act, tot):
        @pl.loop(0, n_tile)
        def _(i):
            wide = jnp.dot(
                feats[...], vector[:, columns(i)], preferred_element_type=jnp.float32
            )
            act[:, columns(i)] = (gate[:, columns(i)].astype(jnp.float32) * wide).astype(
                jnp.bfloat16
            )
            tot[:, columns(i)] = jnp.zeros_like(wide)

    def product(slot, p, act):
        partial_sum = lax.dot_general(
            act[...], weights[span(p), :], (((1,), (1,)), ((), ())),
            preferred_element_type=jnp.float32,
        )
        part1[slot] = partial_sum.astype(jnp.bfloat16).reshape(n_tp, rows, UNIT)
        for d in range(1, n_tp):
            push(
                part1.at[slot, lax.rem(j_me + d, n_tp)], got1.at[slot, d - 1],
                rs_send1.at[0], rs_recv1.at[slot], peers[d - 1],
            )

    def reduce(slot):
        drained(got1.at[slot], rs_recv1.at[slot])
        added = part1[slot, j_me].astype(jnp.float32)
        for d in range(1, n_tp):
            added = added + got1[slot, d - 1].astype(jnp.float32)
        mixed1[slot, j_me] = added.astype(jnp.bfloat16)
        for peer in peers:
            push(
                mixed1.at[slot, j_me], mixed1.at[slot, j_me],
                ag_send1.at[0], ag_recv1.at[slot], peer,
            )

    def back(slot, p, tot):
        drained(mixed1.at[slot, pl.ds(0, n_tp - 1)], ag_recv1.at[slot])
        tot[...] += jnp.dot(
            mixed1[slot].reshape(tokens, UNIT), weights[span(p), :],
            preferred_element_type=jnp.float32,
        )

    def make_image(vector, image, slot, extra):
        def body(i, carry):
            second = (gated[:, columns(i)].astype(jnp.float32) * total[:, columns(i)]).astype(
                jnp.bfloat16
            )
            outer = lax.dot_general(
                features[...], second, (((0,), (0,)), ((), ())),
                preferred_element_type=jnp.float32,
            )
            if extra is not None:
                outer = outer + extra[i].astype(jnp.float32)
            v = vector[:, columns(i)]
            value = outer / live + rate * v
            image[:, columns(i)] = value
            return carry[0] + v * v, carry[1] + v * value

        zero = jnp.zeros((vector.shape[0], tile), jnp.float32)
        squares, crosses = lax.fori_loop(0, n_tile, body, (zero, zero))
        sums[slot, 0] = jnp.broadcast_to(jnp.sum(squares, keepdims=True), (8, 128))
        sums[slot, 1] = jnp.broadcast_to(jnp.sum(crosses, keepdims=True), (8, 128))
        for d in range(1, n_tp):
            push(
                sums.at[slot], sums_got.at[slot, d - 1],
                sum_send.at[slot], sum_recv.at[slot], peers[d - 1],
            )
        drained(sums_got.at[slot], sum_recv.at[slot])
        norm, cross = sums[slot, 0, 0:1, 0:1], sums[slot, 1, 0:1, 0:1]
        for d in range(1, n_tp):
            norm = norm + sums_got[slot, d - 1, 0, 0:1, 0:1]
            cross = cross + sums_got[slot, d - 1, 1, 0:1, 0:1]
        return norm, cross

    make_active(features, vector16, gated, active, total)
    count = n_unit - subs + inner * subs

    @pl.loop(0, count + 2 * LAG)
    def _(e):
        p, before, earlier = unit_of(e), unit_of(e - LAG), unit_of(e - 2 * LAG)

        @pl.when((e >= LAG) & (e < count + LAG))
        def _():
            @pl.when(before >= 3 * subs)
            def _():
                reduce(before + subs)

            reduce(e - LAG)

        @pl.when(e >= 2 * LAG)
        def _():
            @pl.when(earlier >= 3 * subs)
            def _():
                back(earlier + subs, earlier, far_total)

            back(e - 2 * LAG, earlier, total)

        @pl.when(e < count)
        def _():
            @pl.when(e >= subs)
            def _():
                arrive(p)

            completed(p)

            @pl.when(p >= 3 * subs)
            def _():
                @pl.when(p == n_unit - 1)
                def _():
                    for place, ref in enumerate((far_features, far_vector, far_gated)):
                        drained(ref, far_recv.at[place])
                    make_active(far_features, far_vector, far_gated, far_active, far_total)

                product(p + subs, p, far_active)

            product(e, p, active)

    @pl.when(inner == 1)
    def _():
        @pl.loop(0, n_tile)
        def _(i):
            second = (
                far_gated[:, columns(i)].astype(jnp.float32) * far_total[:, columns(i)]
            ).astype(jnp.bfloat16)
            far_image[i] = lax.dot_general(
                far_features[...], second, (((0,), (0,)), ((), ())),
                preferred_element_type=jnp.float32,
            ).astype(jnp.bfloat16)
            push(far_image.at[i], image_got.at[i], far_send.at[3], far_recv.at[3], outward)

        @pl.loop(0, subs - EARLY)
        def _(s):
            send_half(n_unit - 1 - EARLY - s, outward, out_send)

    @pl.when(inner == 0)
    def _():
        @pl.loop(0, EARLY)
        def _(s):
            arrive(n_unit - 1 - s)

        drained(image_got, far_recv.at[3])

    norm0, cross0 = make_image(grad, image0, 0, image_got)
    alpha0 = norm0 / cross0

    @pl.loop(0, n_tile)
    def _(i):
        value = grad[:, columns(i)] - alpha0 * image0[:, columns(i)]
        res_ref[:, columns(i)] = value
        wide = jnp.dot(
            features[...], value.astype(jnp.bfloat16), preferred_element_type=jnp.float32
        )
        active[:, columns(i)] = (gated[:, columns(i)].astype(jnp.float32) * wide).astype(
            jnp.bfloat16
        )
        total[:, columns(i)] = jnp.zeros_like(wide)

    row, col = j_me // 2, j_me % 2
    beside, below = 2 * row + 1 - col, 2 * (1 - row) + col
    across = n_tp - 1 - j_me
    top, low = pl.ds(0, rows // 2), pl.ds(rows // 2, rows // 2)

    def piece_rows(piece, place):
        return pl.ds(pl.multiple_of(piece * rows + place * (rows // 2), 16), rows // 2)

    side, under = {"task": t_me, "tp": beside}, {"task": t_me, "tp": below}
    early = 3 * subs * UNIT // CHUNK

    def stretch(i):
        c = jnp.where(i < early, i, n_chunk - 1 + early - i)
        start = c * CHUNK + upper * (width - CHUNK - 2 * c * CHUNK)
        return c, pl.ds(pl.multiple_of(start, CHUNK), CHUNK)

    def product2(i):
        c, where = stretch(i)

        @pl.when((inner == 0) & (i >= early))
        def _():
            for p in (2 * c + 1, 2 * c):
                @pl.when(p >= 3 * subs)
                def _(p=p):
                    @pl.when(p < n_unit - EARLY)
                    def _():
                        arrive(p)

                    completed(p)

        partial_sum = lax.dot_general(
            active[...], weights[where, :], (((1,), (1,)), ((), ())),
            preferred_element_type=jnp.float32,
        )
        part2[i] = partial_sum.astype(jnp.bfloat16)
        push(part2.at[i, piece_rows(across, 0)], pass2.at[i, 0], rs_send2.at[0], pass_recv2.at[i], side)
        push(part2.at[i, piece_rows(across, 1)], pass2.at[i, 1], rs_send2.at[0], pass_recv2.at[i], under)
        push(part2.at[i, piece_rows(beside, 0)], got2.at[i, 0, 0], rs_send2.at[0], rs_recv2.at[i], side)
        push(part2.at[i, piece_rows(below, 1)], got2.at[i, 1, 1], rs_send2.at[0], rs_recv2.at[i], under)

    def relay(i):
        drained(pass2.at[i], pass_recv2.at[i])
        for place, piece, target in ((0, below, under), (1, beside, side)):
            added2[i, place] = (
                part2[i, piece_rows(piece, place)].astype(jnp.float32) + pass2[i, place].astype(jnp.float32)
            ).astype(jnp.bfloat16)
            push(
                added2.at[i, place], got2.at[i, 1 - place, place],
                rs_send2.at[0], rs_recv2.at[i], target,
            )

    def reduce2(i):
        drained(got2.at[i], rs_recv2.at[i])
        for place, where in ((0, top), (1, low)):
            mixed2[i, j_me, where] = (
                part2[i, piece_rows(j_me, place)].astype(jnp.float32)
                + got2[i, 0, place].astype(jnp.float32)
                + got2[i, 1, place].astype(jnp.float32)
            ).astype(jnp.bfloat16)
        for target in (side, under):
            push(
                mixed2.at[i, j_me], mixed2.at[i, j_me],
                ag_send2.at[0], ag_recv2.at[i], target,
            )

    def forward2(i):
        drained(mixed2.at[i, pl.ds(0, 2)], ag_recv2.at[i])
        for source, where, target in ((beside, top, under), (below, low, side)):
            piece = mixed2.at[i, source, where]
            push(piece, piece, fw_send.at[0], fw_recv.at[i], target)

    def back2(i):
        _, where = stretch(i)
        drained(mixed2.at[i, 0], fw_recv.at[i])
        total[...] += jnp.dot(
            mixed2[i].reshape(tokens, CHUNK), weights[where, :],
            preferred_element_type=jnp.float32,
        )

    ready = early - (n_chunk - early)

    @pl.loop(0, early)
    def _(i):
        product2(i)

    @pl.loop(0, early)
    def _(i):
        relay(i)

    @pl.loop(0, early)
    def _(i):
        reduce2(i)

    @pl.loop(early, n_chunk)
    def _(i):
        product2(i)

    @pl.loop(early, n_chunk)
    def _(i):
        relay(i)

    @pl.loop(0, early)
    def _(i):
        forward2(i)

    @pl.loop(early, n_chunk)
    def _(i):
        reduce2(i)

    @pl.loop(0, ready)
    def _(i):
        back2(i)

    @pl.loop(early, n_chunk)
    def _(i):
        forward2(i)

    @pl.loop(ready, n_chunk)
    def _(i):
        back2(i)

    norm1, cross1 = make_image(res_ref, image1, 1, None)
    ratio = norm1 / norm0
    alpha1 = norm1 / (cross1 - ratio * norm1 / alpha0)

    @pl.loop(0, n_tile)
    def _(i):
        first, then = grad[:, columns(i)], res_ref[:, columns(i)]
        sol_ref[:, columns(i)] = alpha0 * first + alpha1 * (then + ratio * first)
        res_ref[:, columns(i)] = then - alpha1 * (
            image1[:, columns(i)] + ratio * image0[:, columns(i)]
        )

    drained(weights.at[pl.ds(0, n_unit * HALF)], d2d_send.at[0])
    slots = part1.shape[0]

    @pl.when(inner == 0)
    def _():
        drained(weights.at[pl.ds(0, subs * HALF)], in_send.at[0])
        for place, ref in enumerate((features, vector16, gated)):
            drained(ref, far_send.at[place])
        for sem in (rs_send1, ag_send1):
            drained(got1.at[pl.ds(0, n_unit - subs)], sem.at[0])

    @pl.when(inner == 1)
    def _():
        drained(weights.at[pl.ds(0, 2 * subs * HALF)], in_send.at[0])
        drained(weights.at[pl.ds(0, 3 * subs * HALF)], out_send.at[0])
        drained(far_image, far_send.at[3])
        for sem in (rs_send1, ag_send1):
            drained(got1.at[pl.ds(0, slots)], sem.at[0])

    every = pl.ds(0, n_chunk)
    drained(mixed2.at[every, pl.ds(0, 3)], rs_send2.at[0])
    drained(mixed2.at[every, pl.ds(0, 2)], ag_send2.at[0])
    drained(mixed2.at[every, 0], fw_send.at[0])
    for slot in range(2):
        drained(sums_got.at[slot], sum_send.at[slot])


def fused(n_tp, support_x, adapter_a, gate_pre, lengths, damping, down_w, grad_b):
    tokens, width = support_x.shape[1:]
    rank = adapter_a.shape[2]
    hidden, share = down_w.shape
    subs = share // HALF
    n_unit = 4 * subs
    slots = n_unit + subs
    rows = tokens // n_tp
    n_chunk = width // CHUNK
    tile = next(size for size in (512, 256, 128) if hidden % size == 0)
    f32, bf16 = jnp.float32, jnp.bfloat16
    dma = pltpu.SemaphoreType.DMA
    anywhere, vmem = pl.BlockSpec(memory_space=pl.ANY), pl.BlockSpec(memory_space=pltpu.VMEM)
    smem = pl.BlockSpec(memory_space=pltpu.SMEM)
    shape = jax.ShapeDtypeStruct((rank, hidden), f32)
    solved, residual = pl.pallas_call(
        kernel,
        out_shape=(shape, shape),
        in_specs=[anywhere, anywhere, anywhere, smem, smem, anywhere, anywhere],
        out_specs=(vmem, vmem),
        scratch_shapes=[
            pltpu.VMEM((rank, width), bf16),
            pltpu.VMEM((rank, hidden), f32),
            pltpu.VMEM((width, hidden), bf16),
            pltpu.VMEM((tokens, hidden), bf16),
            pltpu.VMEM((tokens, hidden), bf16),
            pltpu.VMEM((tokens, hidden), f32),
            pltpu.VMEM((tokens, rank), bf16),
            pltpu.VMEM((rank, hidden), f32),
            pltpu.VMEM((rank, hidden), f32),
            pltpu.VMEM((tokens, hidden), bf16),
            pltpu.VMEM((tokens, hidden), bf16),
            pltpu.VMEM((tokens, hidden), f32),
            pltpu.VMEM((tokens, rank), bf16),
            pltpu.VMEM((rank, hidden), bf16),
            pltpu.VMEM((rank, hidden), bf16),
            pltpu.VMEM((hidden // tile, rank, tile), bf16),
            pltpu.VMEM((hidden // tile, rank, tile), bf16),
            pltpu.VMEM((slots, n_tp, rows, UNIT), bf16),
            pltpu.VMEM((slots, n_tp - 1, rows, UNIT), bf16),
            pltpu.VMEM((slots, n_tp, rows, UNIT), bf16),
            pltpu.VMEM((n_chunk, tokens, CHUNK), bf16),
            pltpu.VMEM((n_chunk, 2, rows // 2, CHUNK), bf16),
            pltpu.VMEM((n_chunk, 2, rows // 2, CHUNK), bf16),
            pltpu.VMEM((n_chunk, 2, 2, rows // 2, CHUNK), bf16),
            pltpu.VMEM((n_chunk, n_tp, rows, CHUNK), bf16),
            pltpu.VMEM((2, 2, 8, 128), f32),
            pltpu.VMEM((2, n_tp - 1, 2, 8, 128), f32),
            dma((5,)),
            dma((n_unit,)),
            dma((n_unit,)),
            dma((1,)),
            dma((1,)),
            dma((1,)),
            dma((4,)),
            dma((4,)),
            dma((1,)),
            dma((slots,)),
            dma((1,)),
            dma((slots,)),
            dma((1,)),
            dma((n_chunk,)),
            dma((n_chunk,)),
            dma((1,)),
            dma((n_chunk,)),
            dma((1,)),
            dma((n_chunk,)),
            dma((2,)),
            dma((2,)),
        ],
        compiler_params=pltpu.CompilerParams(
            collective_id=0, has_side_effects=True, vmem_limit_bytes=66_000_000
        ),
    )(
        support_x[0], adapter_a[0].T, gate_pre[0], lengths, damping, down_w.T, grad_b[0]
    )
    return solved[None], residual[None]


def solution(mesh):
    in_specs = (
        P("task", None, None),
        P("task", None, None),
        P("task", None, "tp"),
        P("task"),
        P("task"),
        P("tp", "task"),
        P("task", None, "tp"),
    )
    out_specs = (P("task", None, "tp"), P("task", None, "tp"))
    n_task, n_tp = mesh.shape["task"], mesh.shape["tp"]

    def body(support_x, *rest):
        tokens, width = support_x.shape[1:]
        hidden, share = rest[4].shape
        even = tokens % (32 * n_tp) == 0 and hidden % 128 == 0
        if n_tp != 4 or n_task != 8 or share % HALF or width % CHUNK or not even:
            return shards(support_x, *rest)
        return fused(n_tp, support_x, *rest)

    return jax.shard_map(body, mesh=mesh, in_specs=in_specs, out_specs=out_specs, check_vma=False)
```

```python
import jax
import jax.numpy as jnp
from jax import lax
from jax.experimental import pallas as pl
from jax.experimental.pallas import tpu as pltpu
from jax.sharding import PartitionSpec as P

ITERS = 2


def shards(support_x, adapter_a, gate_pre, lengths, damping, down_w, grad_b):
    down_full = lax.all_gather(down_w, "task", axis=1, tiled=True)
    features = jnp.dot(support_x[0], adapter_a[0], preferred_element_type=jnp.float32).astype(
        jnp.bfloat16
    )
    positions = lax.broadcasted_iota(jnp.int32, (gate_pre.shape[1], 1), 0)
    gated = jnp.where(
        positions < lengths[0], jax.nn.silu(gate_pre[0].astype(jnp.float32)), 0.0
    ).astype(jnp.bfloat16)
    tokens_live = lengths[0].astype(jnp.float32)
    damping_rate = damping[0]

    def transposed(mixed_rows):
        return lax.dot_general(
            mixed_rows, down_full, (((1,), (1,)), ((), ())), preferred_element_type=jnp.float32
        )

    def apply(vector):
        inner = jnp.dot(features, vector.astype(jnp.bfloat16), preferred_element_type=jnp.float32)
        active = (gated * inner).astype(jnp.bfloat16)
        partial_sum = jnp.dot(active, down_full, preferred_element_type=jnp.float32)
        mixed = lax.psum(partial_sum.astype(jnp.bfloat16), "tp")
        second = (gated * transposed(mixed)).astype(jnp.bfloat16)
        product = lax.dot_general(
            features, second, (((0,), (0,)), ((), ())), preferred_element_type=jnp.float32
        )
        return product / tokens_live + damping_rate * vector

    def paired_sums(vector, image):
        return lax.psum((jnp.sum(vector * vector), jnp.sum(vector * image)), "tp")

    target = grad_b[0]
    solution = jnp.zeros_like(target)
    residual = target
    image = apply(residual)
    norm_now, product = paired_sums(residual, image)
    alpha = norm_now / product
    direction, along = (residual, image)
    for step in range(ITERS):
        solution = solution + alpha * direction
        residual = residual - alpha * along
        if step + 1 < ITERS:
            image = apply(residual)
            norm_next, product = paired_sums(residual, image)
            ratio = norm_next / norm_now
            alpha = norm_next / (product - ratio * norm_next / alpha)
            direction = residual + ratio * direction
            along = image + ratio * along
            norm_now = norm_next
    return (solution[None], residual[None])


MESH = pl.DeviceIdType.MESH
HALF = 64
UNIT = 2 * HALF
PAIR = 2 * UNIT
CHUNK = 512
AHEAD = 2
EARLY = 3
LAG = 2


def arrival_order(subs):
    near, far = list(range(subs)), list(range(subs - 1, -1, -1))
    clock, times = 0.0, []
    for place in near:
        if place == AHEAD:
            clock += subs
        clock += 1.0
        times.append((clock, place))
    events = [(when, 0, place) for when, place in times]
    events += [(place + 1.0, 1, 2 * subs + far[place]) for place in near]
    clock = float(subs)
    for when, place in times:
        clock = max(clock, when) + 1.0
        events.append((clock, 2, 3 * subs + far[place]))
    middle = [subs + place for place in near] + [unit for _, _, unit in sorted(events)]
    end = near + [subs + place for place in near] + [2 * subs + place for place in far]
    return [order if len(order) % 2 == 0 else order + order[-1:] for order in (end, middle)]


def far_pairs(order, subs):
    pairs, held, slots = [], [], len(order) // 2
    for e in range(slots):
        held += [unit for unit in order[2 * e : 2 * e + 2] if unit >= 3 * subs]
        take = []
        if len(held) >= 2:
            take = [held.pop(0), held.pop(0)]
        elif held and e >= slots - 2:
            take = [held[0], held.pop(0)]
        pairs.append(take)
    return pairs


def kernel(
    support_hbm, adapter_hbm, gate_hbm, length_ref, damping_ref, w_hbm, grad_hbm,
    sol_ref, res_ref,
    adapter, grad, weights, gated, active, total, features, image0, image1,
    far_gated, far_active, far_total, far_features, vector16, far_vector, far_image, image_got,
    part1, got1, mixed1, part2, pass2, added2, got2, mixed2, sums, sums_got,
    load_sem, w_recv, p_recv, in_send, out_send, d2d_send, far_send, far_recv,
    rs_send1, rs_recv1, ag_send1, ag_recv1, rs_send2, pass_recv2, rs_recv2,
    ag_send2, ag_recv2, fw_send, fw_recv, sum_send, sum_recv,
):
    t_me, j_me = lax.axis_index("task"), lax.axis_index("tp")
    z, core = t_me // 2, t_me % 2
    other = 1 - core
    upper = z // 2
    inner = z + upper * (3 - 2 * z)
    n_tp, rows = part1.shape[1:3]
    tokens, hidden = active.shape
    width = weights.shape[0]
    subs = w_hbm.shape[0] // HALF
    n_unit = 4 * subs
    n_chunk = part2.shape[0]
    tile = far_image.shape[2]
    n_tile = hidden // tile
    ends, middles = arrival_order(subs)
    fars = far_pairs(middles, subs)
    n_far = sum(1 for pair in fars if pair)
    numbers = [sum(1 for pair in fars[:e] if pair) for e in range(len(fars))]
    slots = len(fars)

    def pick(e, table):
        value = table[0]
        for place in range(1, slots):
            if place < len(table):
                value = jnp.where(e == place, table[place], value)
        return value

    def pair_of(e):
        found = []
        for k in range(2):
            first, second = ends[k::2], middles[k::2]
            first = first + first[-1:] * (slots - len(first))
            found.append(pick(e, [f + inner * (g - f) for f, g in zip(first, second)]))
        return found

    def far_of(e):
        return [pick(e, [pair[k] if pair else 0 for pair in fars]) for k in range(2)]

    def far_slot(e):
        return slots + pick(e, numbers)

    def has_far(e):
        return (inner == 1) & (pick(e, [1 if pair else 0 for pair in fars]) == 1)

    def placed(p):
        return p + upper * (n_unit - 1 - 2 * p)

    def half(p, side):
        return weights.at[pl.ds(pl.multiple_of(placed(p) * UNIT + side * HALF, HALF), HALF)]

    def span(p):
        return pl.ds(pl.multiple_of(placed(p) * UNIT, UNIT), UNIT)

    own = [
        pltpu.make_async_copy(
            w_hbm.at[pl.ds(s * HALF, HALF)],
            weights.at[pl.ds(pl.multiple_of((z * subs + s) * UNIT + core * HALF, HALF), HALF)],
            load_sem.at[0],
        )
        for s in range(subs)
    ]
    for load in own:
        load.start()
    loads = [
        pltpu.make_async_copy(source, target, load_sem.at[1 + place])
        for place, (source, target) in enumerate(
            ((gate_hbm, active), (adapter_hbm, adapter), (grad_hbm, grad))
        )
    ] + [
        pltpu.make_async_copy(
            support_hbm.at[:, pl.ds(c * CHUNK, CHUNK)], part2.at[c], load_sem.at[4]
        )
        for c in range(n_chunk)
    ]
    for load in loads:
        load.start()

    inward = {"task": t_me + 2 - 4 * upper, "tp": j_me}
    outward = {"task": t_me - 2 + 4 * upper, "tp": j_me}
    partner = {"task": 2 * z + other, "tp": j_me}
    peers = [{"task": t_me, "tp": lax.rem(j_me + d, n_tp)} for d in range(1, n_tp)]

    barrier = pltpu.get_barrier_semaphore()
    for peer in [partner, inward] + peers:
        pl.semaphore_signal(barrier, inc=1, device_id=peer, device_id_type=MESH)

    @pl.when(inner == 1)
    def _():
        pl.semaphore_signal(barrier, inc=1, device_id=outward, device_id_type=MESH)

    pl.semaphore_wait(barrier, n_tp + 1 + inner)

    def drained(ref, sem):
        pltpu.make_async_copy(ref, ref, sem).wait()

    def push(src, dst, send_sem, recv_sem, target):
        pltpu.make_async_remote_copy(
            src_ref=src, dst_ref=dst, send_sem=send_sem, recv_sem=recv_sem,
            device_id=target, device_id_type=MESH,
        ).start()

    def send_half(p, target, send_sem):
        push(half(p, core), half(p, core), send_sem.at[0], w_recv.at[placed(p)], target)

    def share_half(p):
        push(half(p, core), half(p, core), d2d_send.at[0], p_recv.at[placed(p)], partner)

    def arrive(p):
        drained(half(p, core), w_recv.at[placed(p)])

        @pl.when((inner == 1) & (p < subs))
        def _():
            send_half(p, inward, in_send)

        @pl.when((inner == 1) & (p >= 2 * subs) & ((p < 3 * subs) | (p >= n_unit - EARLY)))
        def _():
            send_half(p, outward, out_send)

        share_half(p)

    def completed(p):
        drained(half(p, other), p_recv.at[placed(p)])

    first = inner * subs
    drained(weights.at[pl.ds(0, subs * HALF)], load_sem.at[0])

    @pl.loop(0, AHEAD)
    def _(s):
        send_half(first + s, inward, in_send)

        @pl.when(inner == 1)
        def _():
            send_half(first + s, outward, out_send)

        share_half(first + s)

    @pl.when(inner == 1)
    def _():
        @pl.loop(AHEAD, subs)
        def _(s):
            send_half(first + s, inward, in_send)
            send_half(first + s, outward, out_send)

    @pl.loop(AHEAD, subs)
    def _(s):
        share_half(first + s)

    loads[1].wait()
    drained(part2, load_sem.at[4])
    wide = jnp.zeros(features.shape, jnp.float32)
    for c in range(n_chunk):
        wide = wide + lax.dot_general(
            part2[c], adapter[:, pl.ds(c * CHUNK, CHUNK)], (((1,), (1,)), ((), ())),
            preferred_element_type=jnp.float32,
        )
    features[...] = wide.astype(jnp.bfloat16)
    loads[0].wait()
    loads[2].wait()
    live, rate = length_ref[0].astype(jnp.float32), damping_ref[0]
    positions = lax.broadcasted_iota(jnp.int32, (tokens, tile), 0).astype(jnp.float32)

    def columns(i):
        return pl.ds(pl.multiple_of(i * tile, tile), tile)

    @pl.loop(0, n_tile, unroll=True)
    def _(i):
        pre = active[:, columns(i)].astype(jnp.float32)
        gated[:, columns(i)] = jnp.where(
            positions < live, pre / (1.0 + jnp.exp(-pre)), 0.0
        ).astype(jnp.bfloat16)
        vector16[:, columns(i)] = grad[:, columns(i)].astype(jnp.bfloat16)

    @pl.when(inner == 0)
    def _():
        for place, (src, dst) in enumerate(
            ((features, far_features), (vector16, far_vector), (gated, far_gated))
        ):
            push(src, dst, far_send.at[place], far_recv.at[place], inward)

        @pl.loop(AHEAD, subs)
        def _(s):
            send_half(first + s, inward, in_send)

    @pl.when(inner == 1)
    def _():
        image_got[...] = jnp.zeros_like(image_got)

    def make_active(feats, vector, gate, act, tot):
        @pl.loop(0, n_tile, unroll=True)
        def _(i):
            wide = jnp.dot(
                feats[...], vector[:, columns(i)], preferred_element_type=jnp.float32
            )
            act[:, columns(i)] = (gate[:, columns(i)].astype(jnp.float32) * wide).astype(
                jnp.bfloat16
            )
            tot[:, columns(i)] = jnp.zeros_like(wide)

    def pair_rows(pair):
        return jnp.concatenate([weights[span(pair[0]), :], weights[span(pair[1]), :]], axis=0)

    def product(slot, pair, act):
        partial_sum = lax.dot_general(
            act[...], pair_rows(pair), (((1,), (1,)), ((), ())),
            preferred_element_type=jnp.float32,
        )
        lanes = lax.broadcasted_iota(jnp.int32, partial_sum.shape, 1)
        kept = jnp.where(pair[0] == pair[1], UNIT, PAIR)
        partial_sum = jnp.where(lanes < kept, partial_sum, 0.0)
        part1[slot] = partial_sum.astype(jnp.bfloat16).reshape(n_tp, rows, PAIR)
        for d in range(1, n_tp):
            push(
                part1.at[slot, lax.rem(j_me + d, n_tp)], got1.at[slot, d - 1],
                rs_send1.at[0], rs_recv1.at[slot], peers[d - 1],
            )

    def reduce(slot):
        drained(got1.at[slot], rs_recv1.at[slot])
        added = part1[slot, j_me].astype(jnp.float32)
        for d in range(1, n_tp):
            added = added + got1[slot, d - 1].astype(jnp.float32)
        mixed1[slot, j_me] = added.astype(jnp.bfloat16)
        for peer in peers:
            push(
                mixed1.at[slot, j_me], mixed1.at[slot, j_me],
                ag_send1.at[0], ag_recv1.at[slot], peer,
            )

    def back(slot, pair, tot):
        drained(mixed1.at[slot, pl.ds(0, n_tp - 1)], ag_recv1.at[slot])
        tot[...] += jnp.dot(
            mixed1[slot].reshape(tokens, PAIR), pair_rows(pair),
            preferred_element_type=jnp.float32,
        )

    def make_image(vector, image, slot, extra):
        def body(i, carry):
            second = (gated[:, columns(i)].astype(jnp.float32) * total[:, columns(i)]).astype(
                jnp.bfloat16
            )
            outer = lax.dot_general(
                features[...], second, (((0,), (0,)), ((), ())),
                preferred_element_type=jnp.float32,
            )
            if extra is not None:
                outer = outer + extra[i].astype(jnp.float32)
            v = vector[:, columns(i)]
            value = outer / live + rate * v
            image[:, columns(i)] = value
            return carry[0] + v * v, carry[1] + v * value

        zero = jnp.zeros((vector.shape[0], tile), jnp.float32)
        squares, crosses = lax.fori_loop(0, n_tile, body, (zero, zero), unroll=True)
        sums[slot, 0] = jnp.broadcast_to(jnp.sum(squares, keepdims=True), (8, 128))
        sums[slot, 1] = jnp.broadcast_to(jnp.sum(crosses, keepdims=True), (8, 128))
        for d in range(1, n_tp):
            push(
                sums.at[slot], sums_got.at[slot, d - 1],
                sum_send.at[slot], sum_recv.at[slot], peers[d - 1],
            )
        drained(sums_got.at[slot], sum_recv.at[slot])
        norm, cross = sums[slot, 0, 0:1, 0:1], sums[slot, 1, 0:1, 0:1]
        for d in range(1, n_tp):
            norm = norm + sums_got[slot, d - 1, 0, 0:1, 0:1]
            cross = cross + sums_got[slot, d - 1, 1, 0:1, 0:1]
        return norm, cross

    make_active(features, vector16, gated, active, total)
    short = len(ends) // 2
    count = short + inner * (slots - short)

    @pl.loop(0, count + 2 * LAG)
    def _(e):
        @pl.when((e >= LAG) & (e < count + LAG))
        def _():
            @pl.when(has_far(e - LAG))
            def _():
                reduce(far_slot(e - LAG))

            reduce(e - LAG)

        @pl.when(e >= 2 * LAG)
        def _():
            @pl.when(has_far(e - 2 * LAG))
            def _():
                back(far_slot(e - 2 * LAG), far_of(e - 2 * LAG), far_total)

            @pl.when(e < count)
            def _():
                back(e - 2 * LAG, pair_of(e - 2 * LAG), total)

        @pl.when(e < count)
        def _():
            pair = pair_of(e)
            for k, p in enumerate(pair):
                @pl.when((2 * e + k >= subs) & ((k == 0) | (pair[0] != pair[1])))
                def _(p=p):
                    arrive(p)

            for k, p in enumerate(pair):
                @pl.when((k == 0) | (pair[0] != pair[1]))
                def _(p=p):
                    completed(p)

            @pl.when(has_far(e))
            def _():
                @pl.when(far_slot(e) == slots)
                def _():
                    for place, ref in enumerate((far_features, far_vector, far_gated)):
                        drained(ref, far_recv.at[place])
                    make_active(far_features, far_vector, far_gated, far_active, far_total)

                product(far_slot(e), far_of(e), far_active)

            product(e, pair, active)

    @pl.when(inner == 1)
    def _():
        @pl.loop(0, n_tile, unroll=True)
        def _(i):
            second = (
                far_gated[:, columns(i)].astype(jnp.float32) * far_total[:, columns(i)]
            ).astype(jnp.bfloat16)
            far_image[i] = lax.dot_general(
                far_features[...], second, (((0,), (0,)), ((), ())),
                preferred_element_type=jnp.float32,
            ).astype(jnp.bfloat16)
            push(far_image.at[i], image_got.at[i], far_send.at[3], far_recv.at[3], outward)

        @pl.loop(0, subs - EARLY)
        def _(s):
            send_half(n_unit - 1 - EARLY - s, outward, out_send)

    @pl.loop(count - 2 * LAG, count)
    def _(e):
        back(e, pair_of(e), total)

    @pl.when(inner == 0)
    def _():
        @pl.loop(0, EARLY)
        def _(s):
            arrive(n_unit - 1 - s)

        drained(image_got, far_recv.at[3])

    norm0, cross0 = make_image(grad, image0, 0, image_got)
    alpha0 = norm0 / cross0

    @pl.loop(0, n_tile, unroll=True)
    def _(i):
        value = grad[:, columns(i)] - alpha0 * image0[:, columns(i)]
        res_ref[:, columns(i)] = value
        wide = jnp.dot(
            features[...], value.astype(jnp.bfloat16), preferred_element_type=jnp.float32
        )
        active[:, columns(i)] = (gated[:, columns(i)].astype(jnp.float32) * wide).astype(
            jnp.bfloat16
        )
        total[:, columns(i)] = jnp.zeros_like(wide)

    row, col = j_me // 2, j_me % 2
    beside, below = 2 * row + 1 - col, 2 * (1 - row) + col
    across = n_tp - 1 - j_me
    top, low = pl.ds(0, rows // 2), pl.ds(rows // 2, rows // 2)

    def piece_rows(piece, place):
        return pl.ds(pl.multiple_of(piece * rows + place * (rows // 2), 16), rows // 2)

    side, under = {"task": t_me, "tp": beside}, {"task": t_me, "tp": below}
    early = 3 * subs * UNIT // CHUNK

    def stretch(i):
        c = jnp.where(i < early, i, n_chunk - 1 + early - i)
        start = c * CHUNK + upper * (width - CHUNK - 2 * c * CHUNK)
        return c, pl.ds(pl.multiple_of(start, CHUNK), CHUNK)

    def product2(i):
        c, where = stretch(i)

        @pl.when((inner == 0) & (i >= early))
        def _():
            for k in range(CHUNK // UNIT - 1, -1, -1):
                p = CHUNK // UNIT * c + k

                @pl.when(p >= 3 * subs)
                def _(p=p):
                    @pl.when(p < n_unit - EARLY)
                    def _():
                        arrive(p)

                    completed(p)

        partial_sum = lax.dot_general(
            active[...], weights[where, :], (((1,), (1,)), ((), ())),
            preferred_element_type=jnp.float32,
        )
        part2[i] = partial_sum.astype(jnp.bfloat16)
        push(part2.at[i, piece_rows(across, 0)], pass2.at[i, 0], rs_send2.at[0], pass_recv2.at[i], side)
        push(part2.at[i, piece_rows(across, 1)], pass2.at[i, 1], rs_send2.at[0], pass_recv2.at[i], under)
        push(part2.at[i, piece_rows(beside, 0)], got2.at[i, 0, 0], rs_send2.at[0], rs_recv2.at[i], side)
        push(part2.at[i, piece_rows(below, 1)], got2.at[i, 1, 1], rs_send2.at[0], rs_recv2.at[i], under)

    def relay(i):
        drained(pass2.at[i], pass_recv2.at[i])
        for place, piece, target in ((0, below, under), (1, beside, side)):
            added2[i, place] = (
                part2[i, piece_rows(piece, place)].astype(jnp.float32) + pass2[i, place].astype(jnp.float32)
            ).astype(jnp.bfloat16)
            push(
                added2.at[i, place], got2.at[i, 1 - place, place],
                rs_send2.at[0], rs_recv2.at[i], target,
            )

    def reduce2(i):
        drained(got2.at[i], rs_recv2.at[i])
        for place, where in ((0, top), (1, low)):
            mixed2[i, j_me, where] = (
                part2[i, piece_rows(j_me, place)].astype(jnp.float32)
                + got2[i, 0, place].astype(jnp.float32)
                + got2[i, 1, place].astype(jnp.float32)
            ).astype(jnp.bfloat16)
        for target in (side, under):
            push(
                mixed2.at[i, j_me], mixed2.at[i, j_me],
                ag_send2.at[0], ag_recv2.at[i], target,
            )

    def forward2(i):
        drained(mixed2.at[i, pl.ds(0, 2)], ag_recv2.at[i])
        for source, where, target in ((beside, top, under), (below, low, side)):
            piece = mixed2.at[i, source, where]
            push(piece, piece, fw_send.at[0], fw_recv.at[i], target)

    def back2(i):
        _, where = stretch(i)
        drained(mixed2.at[i, 0], fw_recv.at[i])
        total[...] += jnp.dot(
            mixed2[i].reshape(tokens, CHUNK), weights[where, :],
            preferred_element_type=jnp.float32,
        )

    ready = early - (n_chunk - early)

    @pl.loop(0, early)
    def _(i):
        product2(i)

    @pl.loop(0, early)
    def _(i):
        relay(i)

    @pl.loop(0, early)
    def _(i):
        reduce2(i)

    @pl.loop(early, n_chunk)
    def _(i):
        product2(i)

    @pl.loop(early, n_chunk)
    def _(i):
        relay(i)

    @pl.loop(0, early)
    def _(i):
        forward2(i)

    @pl.loop(early, n_chunk)
    def _(i):
        reduce2(i)

    @pl.loop(0, ready)
    def _(i):
        back2(i)

    @pl.loop(early, n_chunk)
    def _(i):
        forward2(i)

    @pl.loop(ready, n_chunk)
    def _(i):
        back2(i)

    norm1, cross1 = make_image(res_ref, image1, 1, None)
    ratio = norm1 / norm0
    alpha1 = norm1 / (cross1 - ratio * norm1 / alpha0)

    @pl.loop(0, n_tile, unroll=True)
    def _(i):
        first, then = grad[:, columns(i)], res_ref[:, columns(i)]
        sol_ref[:, columns(i)] = alpha0 * first + alpha1 * (then + ratio * first)
        res_ref[:, columns(i)] = then - alpha1 * (
            image1[:, columns(i)] + ratio * image0[:, columns(i)]
        )

    drained(weights.at[pl.ds(0, n_unit * HALF)], d2d_send.at[0])

    @pl.when(inner == 0)
    def _():
        drained(weights.at[pl.ds(0, subs * HALF)], in_send.at[0])
        for place, ref in enumerate((features, vector16, gated)):
            drained(ref, far_send.at[place])
        for sem in (rs_send1, ag_send1):
            drained(got1.at[pl.ds(0, short)], sem.at[0])

    @pl.when(inner == 1)
    def _():
        drained(weights.at[pl.ds(0, 2 * subs * HALF)], in_send.at[0])
        drained(weights.at[pl.ds(0, 3 * subs * HALF)], out_send.at[0])
        drained(far_image, far_send.at[3])
        for sem in (rs_send1, ag_send1):
            drained(got1.at[pl.ds(0, slots + n_far)], sem.at[0])

    every = pl.ds(0, n_chunk)
    drained(mixed2.at[every, pl.ds(0, 3)], rs_send2.at[0])
    drained(mixed2.at[every, pl.ds(0, 2)], ag_send2.at[0])
    drained(mixed2.at[every, 0], fw_send.at[0])
    for slot in range(2):
        drained(sums_got.at[slot], sum_send.at[slot])


def fused(n_tp, support_x, adapter_a, gate_pre, lengths, damping, down_w, grad_b):
    tokens, width = support_x.shape[1:]
    rank = adapter_a.shape[2]
    hidden, share = down_w.shape
    subs = share // HALF
    n_unit = 4 * subs
    middle = arrival_order(subs)[1]
    slots = len(middle) // 2 + sum(1 for pair in far_pairs(middle, subs) if pair)
    rows = tokens // n_tp
    n_chunk = width // CHUNK
    tile = next(size for size in (512, 256, 128) if hidden % size == 0)
    f32, bf16 = jnp.float32, jnp.bfloat16
    dma = pltpu.SemaphoreType.DMA
    anywhere, vmem = pl.BlockSpec(memory_space=pl.ANY), pl.BlockSpec(memory_space=pltpu.VMEM)
    smem = pl.BlockSpec(memory_space=pltpu.SMEM)
    shape = jax.ShapeDtypeStruct((rank, hidden), f32)
    solved, residual = pl.pallas_call(
        kernel,
        out_shape=(shape, shape),
        in_specs=[anywhere, anywhere, anywhere, smem, smem, anywhere, anywhere],
        out_specs=(vmem, vmem),
        scratch_shapes=[
            pltpu.VMEM((rank, width), bf16),
            pltpu.VMEM((rank, hidden), f32),
            pltpu.VMEM((width, hidden), bf16),
            pltpu.VMEM((tokens, hidden), bf16),
            pltpu.VMEM((tokens, hidden), bf16),
            pltpu.VMEM((tokens, hidden), f32),
            pltpu.VMEM((tokens, rank), bf16),
            pltpu.VMEM((rank, hidden), f32),
            pltpu.VMEM((rank, hidden), f32),
            pltpu.VMEM((tokens, hidden), bf16),
            pltpu.VMEM((tokens, hidden), bf16),
            pltpu.VMEM((tokens, hidden), f32),
            pltpu.VMEM((tokens, rank), bf16),
            pltpu.VMEM((rank, hidden), bf16),
            pltpu.VMEM((rank, hidden), bf16),
            pltpu.VMEM((hidden // tile, rank, tile), bf16),
            pltpu.VMEM((hidden // tile, rank, tile), bf16),
            pltpu.VMEM((slots, n_tp, rows, PAIR), bf16),
            pltpu.VMEM((slots, n_tp - 1, rows, PAIR), bf16),
            pltpu.VMEM((slots, n_tp, rows, PAIR), bf16),
            pltpu.VMEM((n_chunk, tokens, CHUNK), bf16),
            pltpu.VMEM((n_chunk, 2, rows // 2, CHUNK), bf16),
            pltpu.VMEM((n_chunk, 2, rows // 2, CHUNK), bf16),
            pltpu.VMEM((n_chunk, 2, 2, rows // 2, CHUNK), bf16),
            pltpu.VMEM((n_chunk, n_tp, rows, CHUNK), bf16),
            pltpu.VMEM((2, 2, 8, 128), f32),
            pltpu.VMEM((2, n_tp - 1, 2, 8, 128), f32),
            dma((5,)),
            dma((n_unit,)),
            dma((n_unit,)),
            dma((1,)),
            dma((1,)),
            dma((1,)),
            dma((4,)),
            dma((4,)),
            dma((1,)),
            dma((slots,)),
            dma((1,)),
            dma((slots,)),
            dma((1,)),
            dma((n_chunk,)),
            dma((n_chunk,)),
            dma((1,)),
            dma((n_chunk,)),
            dma((1,)),
            dma((n_chunk,)),
            dma((2,)),
            dma((2,)),
        ],
        compiler_params=pltpu.CompilerParams(
            collective_id=0, has_side_effects=True, vmem_limit_bytes=66_000_000
        ),
    )(
        support_x[0], adapter_a[0].T, gate_pre[0], lengths, damping, down_w.T, grad_b[0]
    )
    return solved[None], residual[None]


def solution(mesh):
    in_specs = (
        P("task", None, None),
        P("task", None, None),
        P("task", None, "tp"),
        P("task"),
        P("task"),
        P("tp", "task"),
        P("task", None, "tp"),
    )
    out_specs = (P("task", None, "tp"), P("task", None, "tp"))
    n_task, n_tp = mesh.shape["task"], mesh.shape["tp"]

    def body(support_x, *rest):
        tokens, width = support_x.shape[1:]
        hidden, share = rest[4].shape
        even = tokens % (32 * n_tp) == 0 and hidden % 128 == 0
        if n_tp != 4 or n_task != 8 or share % HALF or width % CHUNK or not even:
            return shards(support_x, *rest)
        return fused(n_tp, support_x, *rest)

    return jax.shard_map(body, mesh=mesh, in_specs=in_specs, out_specs=out_specs, check_vma=False)
```

```python
import jax
import jax.numpy as jnp
from jax import lax
from jax.experimental import pallas as pl
from jax.experimental.pallas import tpu as pltpu
from jax.sharding import PartitionSpec as P

ITERS = 2


def shards(support_x, adapter_a, gate_pre, lengths, damping, down_w, grad_b):
    down_full = lax.all_gather(down_w, "task", axis=1, tiled=True)
    features = jnp.dot(support_x[0], adapter_a[0], preferred_element_type=jnp.float32).astype(
        jnp.bfloat16
    )
    positions = lax.broadcasted_iota(jnp.int32, (gate_pre.shape[1], 1), 0)
    gated = jnp.where(
        positions < lengths[0], jax.nn.silu(gate_pre[0].astype(jnp.float32)), 0.0
    ).astype(jnp.bfloat16)
    tokens_live = lengths[0].astype(jnp.float32)
    damping_rate = damping[0]

    def transposed(mixed_rows):
        return lax.dot_general(
            mixed_rows, down_full, (((1,), (1,)), ((), ())), preferred_element_type=jnp.float32
        )

    def apply(vector):
        inner = jnp.dot(features, vector.astype(jnp.bfloat16), preferred_element_type=jnp.float32)
        active = (gated * inner).astype(jnp.bfloat16)
        partial_sum = jnp.dot(active, down_full, preferred_element_type=jnp.float32)
        mixed = lax.psum(partial_sum.astype(jnp.bfloat16), "tp")
        second = (gated * transposed(mixed)).astype(jnp.bfloat16)
        product = lax.dot_general(
            features, second, (((0,), (0,)), ((), ())), preferred_element_type=jnp.float32
        )
        return product / tokens_live + damping_rate * vector

    def paired_sums(vector, image):
        return lax.psum((jnp.sum(vector * vector), jnp.sum(vector * image)), "tp")

    target = grad_b[0]
    solution = jnp.zeros_like(target)
    residual = target
    image = apply(residual)
    norm_now, product = paired_sums(residual, image)
    alpha = norm_now / product
    direction, along = (residual, image)
    for step in range(ITERS):
        solution = solution + alpha * direction
        residual = residual - alpha * along
        if step + 1 < ITERS:
            image = apply(residual)
            norm_next, product = paired_sums(residual, image)
            ratio = norm_next / norm_now
            alpha = norm_next / (product - ratio * norm_next / alpha)
            direction = residual + ratio * direction
            along = image + ratio * along
            norm_now = norm_next
    return (solution[None], residual[None])


MESH = pl.DeviceIdType.MESH
HALF = 64
UNIT = 2 * HALF
PAIR = 2 * UNIT
CHUNK = 512
AHEAD = 2
EARLY = 3
LAG = 2


def arrival_order(subs):
    near, far = list(range(subs)), list(range(subs - 1, -1, -1))
    clock, times = 0.0, []
    for place in near:
        if place == AHEAD:
            clock += subs
        clock += 1.0
        times.append((clock, place))
    events = [(when, 0, place) for when, place in times]
    events += [(place + 1.0, 1, 2 * subs + far[place]) for place in near]
    clock = float(subs)
    for when, place in times:
        clock = max(clock, when) + 1.0
        events.append((clock, 2, 3 * subs + far[place]))
    middle = [subs + place for place in near] + [unit for _, _, unit in sorted(events)]
    end = near + [subs + place for place in near] + [2 * subs + place for place in far]
    return [order if len(order) % 2 == 0 else order + order[-1:] for order in (end, middle)]


def far_pairs(order, subs):
    pairs, held, slots = [], [], len(order) // 2
    for e in range(slots):
        held += [unit for unit in order[2 * e : 2 * e + 2] if unit >= 3 * subs]
        take = []
        if len(held) >= 2:
            take = [held.pop(0), held.pop(0)]
        elif held and e >= slots - 2:
            take = [held[0], held.pop(0)]
        pairs.append(take)
    return pairs


def kernel(
    support_hbm, adapter_hbm, gate_hbm, length_ref, damping_ref, w_hbm, grad_hbm,
    sol_ref, res_ref,
    adapter, grad, weights, gated, active, total, features, image0, image1,
    far_gated, far_active, far_total, far_features, vector16, far_vector, far_image, image_got,
    part1, got1, mixed1, part2, pass2, added2, got2, mixed2, sums, sums_got,
    load_sem, w_recv, p_recv, in_send, out_send, d2d_send, far_send, far_recv,
    rs_send1, rs_recv1, ag_send1, ag_recv1, rs_send2, pass_recv2, rs_recv2,
    ag_send2, ag_recv2, fw_send, fw_recv, sum_send, sum_recv,
):
    t_me, j_me = lax.axis_index("task"), lax.axis_index("tp")
    z, core = t_me // 2, t_me % 2
    other = 1 - core
    upper = z // 2
    inner = z + upper * (3 - 2 * z)
    n_tp, rows = part1.shape[1:3]
    tokens, hidden = active.shape
    width = weights.shape[0]
    subs = w_hbm.shape[0] // HALF
    n_unit = 4 * subs
    n_chunk = part2.shape[0]
    tile = far_image.shape[2]
    n_tile = hidden // tile
    ends, middles = arrival_order(subs)
    fars = far_pairs(middles, subs)
    n_far = sum(1 for pair in fars if pair)
    numbers = [sum(1 for pair in fars[:e] if pair) for e in range(len(fars))]
    slots = len(fars)

    def pick(e, table):
        value = table[0]
        for place in range(1, slots):
            if place < len(table):
                value = jnp.where(e == place, table[place], value)
        return value

    def pair_of(e):
        found = []
        for k in range(2):
            first, second = ends[k::2], middles[k::2]
            first = first + first[-1:] * (slots - len(first))
            found.append(pick(e, [f + inner * (g - f) for f, g in zip(first, second)]))
        return found

    def far_of(e):
        return [pick(e, [pair[k] if pair else 0 for pair in fars]) for k in range(2)]

    def far_slot(e):
        return slots + pick(e, numbers)

    def has_far(e):
        return (inner == 1) & (pick(e, [1 if pair else 0 for pair in fars]) == 1)

    def placed(p):
        return p + upper * (n_unit - 1 - 2 * p)

    def half(p, side):
        return weights.at[pl.ds(pl.multiple_of(placed(p) * UNIT + side * HALF, HALF), HALF)]

    def span(p):
        return pl.ds(pl.multiple_of(placed(p) * UNIT, UNIT), UNIT)

    own = [
        pltpu.make_async_copy(
            w_hbm.at[pl.ds(s * HALF, HALF)],
            weights.at[pl.ds(pl.multiple_of((z * subs + s) * UNIT + core * HALF, HALF), HALF)],
            load_sem.at[0],
        )
        for s in range(subs)
    ]
    for load in own:
        load.start()
    loads = [
        pltpu.make_async_copy(source, target, load_sem.at[1 + place])
        for place, (source, target) in enumerate(
            ((gate_hbm, active), (adapter_hbm, adapter), (grad_hbm, grad))
        )
    ] + [
        pltpu.make_async_copy(
            support_hbm.at[:, pl.ds(c * CHUNK, CHUNK)], part2.at[c], load_sem.at[4]
        )
        for c in range(n_chunk)
    ]
    for load in loads:
        load.start()

    inward = {"task": t_me + 2 - 4 * upper, "tp": j_me}
    outward = {"task": t_me - 2 + 4 * upper, "tp": j_me}
    partner = {"task": 2 * z + other, "tp": j_me}
    peers = [{"task": t_me, "tp": lax.rem(j_me + d, n_tp)} for d in range(1, n_tp)]

    barrier = pltpu.get_barrier_semaphore()
    for peer in [partner, inward] + peers:
        pl.semaphore_signal(barrier, inc=1, device_id=peer, device_id_type=MESH)

    @pl.when(inner == 1)
    def _():
        pl.semaphore_signal(barrier, inc=1, device_id=outward, device_id_type=MESH)

    pl.semaphore_wait(barrier, n_tp + 1 + inner)

    def drained(ref, sem):
        pltpu.make_async_copy(ref, ref, sem).wait()

    def push(src, dst, send_sem, recv_sem, target):
        pltpu.make_async_remote_copy(
            src_ref=src, dst_ref=dst, send_sem=send_sem, recv_sem=recv_sem,
            device_id=target, device_id_type=MESH,
        ).start()

    def send_half(p, target, send_sem):
        push(half(p, core), half(p, core), send_sem.at[0], w_recv.at[placed(p)], target)

    def share_half(p):
        push(half(p, core), half(p, core), d2d_send.at[0], p_recv.at[placed(p)], partner)

    def arrive(p):
        drained(half(p, core), w_recv.at[placed(p)])

        @pl.when((inner == 1) & (p < subs))
        def _():
            send_half(p, inward, in_send)

        @pl.when((inner == 1) & (p >= 2 * subs) & ((p < 3 * subs) | (p >= n_unit - EARLY)))
        def _():
            send_half(p, outward, out_send)

        share_half(p)

    def completed(p):
        drained(half(p, other), p_recv.at[placed(p)])

    first = inner * subs
    drained(weights.at[pl.ds(0, subs * HALF)], load_sem.at[0])

    @pl.loop(0, AHEAD)
    def _(s):
        send_half(first + s, inward, in_send)

        @pl.when(inner == 1)
        def _():
            send_half(first + s, outward, out_send)

        share_half(first + s)

    @pl.when(inner == 1)
    def _():
        @pl.loop(AHEAD, subs)
        def _(s):
            send_half(first + s, inward, in_send)
            send_half(first + s, outward, out_send)

    @pl.loop(AHEAD, subs)
    def _(s):
        share_half(first + s)

    loads[1].wait()
    drained(part2, load_sem.at[4])
    wide = jnp.zeros(features.shape, jnp.float32)
    for c in range(n_chunk):
        wide = wide + lax.dot_general(
            part2[c], adapter[:, pl.ds(c * CHUNK, CHUNK)], (((1,), (1,)), ((), ())),
            preferred_element_type=jnp.float32,
        )
    features[...] = wide.astype(jnp.bfloat16)
    loads[0].wait()
    loads[2].wait()
    live, rate = length_ref[0].astype(jnp.float32), damping_ref[0]
    positions = lax.broadcasted_iota(jnp.int32, (tokens, tile), 0).astype(jnp.float32)

    def columns(i):
        return pl.ds(pl.multiple_of(i * tile, tile), tile)

    @pl.loop(0, n_tile, unroll=True)
    def _(i):
        pre = active[:, columns(i)].astype(jnp.float32)
        gated[:, columns(i)] = jnp.where(
            positions < live, pre / (1.0 + jnp.exp(-pre)), 0.0
        ).astype(jnp.bfloat16)
        vector16[:, columns(i)] = grad[:, columns(i)].astype(jnp.bfloat16)

    @pl.when(inner == 0)
    def _():
        for place, (src, dst) in enumerate(
            ((features, far_features), (vector16, far_vector), (gated, far_gated))
        ):
            push(src, dst, far_send.at[place], far_recv.at[place], inward)

        @pl.loop(AHEAD, subs)
        def _(s):
            send_half(first + s, inward, in_send)

    @pl.when(inner == 1)
    def _():
        image_got[...] = jnp.zeros_like(image_got)

    def make_active(feats, vector, gate, act, tot):
        @pl.loop(0, n_tile, unroll=True)
        def _(i):
            wide = jnp.dot(
                feats[...], vector[:, columns(i)], preferred_element_type=jnp.float32
            )
            act[:, columns(i)] = (gate[:, columns(i)].astype(jnp.float32) * wide).astype(
                jnp.bfloat16
            )
            tot[:, columns(i)] = jnp.zeros_like(wide)

    def pair_rows(pair):
        return jnp.concatenate([weights[span(pair[0]), :], weights[span(pair[1]), :]], axis=0)

    def product(slot, pair, act):
        partial_sum = lax.dot_general(
            act[...], pair_rows(pair), (((1,), (1,)), ((), ())),
            preferred_element_type=jnp.float32,
        )
        lanes = lax.broadcasted_iota(jnp.int32, partial_sum.shape, 1)
        kept = jnp.where(pair[0] == pair[1], UNIT, PAIR)
        partial_sum = jnp.where(lanes < kept, partial_sum, 0.0)
        part1[slot] = partial_sum.astype(jnp.bfloat16).reshape(n_tp, rows, PAIR)
        for d in range(1, n_tp):
            push(
                part1.at[slot, lax.rem(j_me + d, n_tp)], got1.at[slot, d - 1],
                rs_send1.at[0], rs_recv1.at[slot], peers[d - 1],
            )

    def reduce(slot):
        drained(got1.at[slot], rs_recv1.at[slot])
        added = part1[slot, j_me].astype(jnp.float32)
        for d in range(1, n_tp):
            added = added + got1[slot, d - 1].astype(jnp.float32)
        mixed1[slot, j_me] = added.astype(jnp.bfloat16)
        for peer in peers:
            push(
                mixed1.at[slot, j_me], mixed1.at[slot, j_me],
                ag_send1.at[0], ag_recv1.at[slot], peer,
            )

    def back(slot, pair, tot):
        drained(mixed1.at[slot, pl.ds(0, n_tp - 1)], ag_recv1.at[slot])
        tot[...] += jnp.dot(
            mixed1[slot].reshape(tokens, PAIR), pair_rows(pair),
            preferred_element_type=jnp.float32,
        )

    def make_image(vector, image, slot, extra):
        def body(i, carry):
            second = (gated[:, columns(i)].astype(jnp.float32) * total[:, columns(i)]).astype(
                jnp.bfloat16
            )
            outer = lax.dot_general(
                features[...], second, (((0,), (0,)), ((), ())),
                preferred_element_type=jnp.float32,
            )
            if extra is not None:
                outer = outer + extra[i].astype(jnp.float32)
            v = vector[:, columns(i)]
            value = outer / live + rate * v
            image[:, columns(i)] = value
            return carry[0] + v * v, carry[1] + v * value

        zero = jnp.zeros((vector.shape[0], tile), jnp.float32)
        squares, crosses = lax.fori_loop(0, n_tile, body, (zero, zero), unroll=True)
        sums[slot, 0] = jnp.broadcast_to(jnp.sum(squares, keepdims=True), (8, 128))
        sums[slot, 1] = jnp.broadcast_to(jnp.sum(crosses, keepdims=True), (8, 128))
        for d in range(1, n_tp):
            push(
                sums.at[slot], sums_got.at[slot, d - 1],
                sum_send.at[slot], sum_recv.at[slot], peers[d - 1],
            )
        drained(sums_got.at[slot], sum_recv.at[slot])
        norm, cross = sums[slot, 0, 0:1, 0:1], sums[slot, 1, 0:1, 0:1]
        for d in range(1, n_tp):
            norm = norm + sums_got[slot, d - 1, 0, 0:1, 0:1]
            cross = cross + sums_got[slot, d - 1, 1, 0:1, 0:1]
        return norm, cross

    make_active(features, vector16, gated, active, total)
    short = len(ends) // 2
    count = short + inner * (slots - short)

    @pl.loop(0, count + 2 * LAG)
    def _(e):
        @pl.when((e >= LAG) & (e < count + LAG))
        def _():
            @pl.when(has_far(e - LAG))
            def _():
                reduce(far_slot(e - LAG))

            reduce(e - LAG)

        @pl.when(e >= 2 * LAG)
        def _():
            @pl.when(has_far(e - 2 * LAG))
            def _():
                back(far_slot(e - 2 * LAG), far_of(e - 2 * LAG), far_total)

            @pl.when(e < count)
            def _():
                back(e - 2 * LAG, pair_of(e - 2 * LAG), total)

        @pl.when(e < count)
        def _():
            pair = pair_of(e)
            for k, p in enumerate(pair):
                @pl.when((2 * e + k >= subs) & ((k == 0) | (pair[0] != pair[1])))
                def _(p=p):
                    arrive(p)

            for k, p in enumerate(pair):
                @pl.when((k == 0) | (pair[0] != pair[1]))
                def _(p=p):
                    completed(p)

            @pl.when(has_far(e))
            def _():
                @pl.when(far_slot(e) == slots)
                def _():
                    for place, ref in enumerate((far_features, far_vector, far_gated)):
                        drained(ref, far_recv.at[place])
                    make_active(far_features, far_vector, far_gated, far_active, far_total)

                product(far_slot(e), far_of(e), far_active)

            product(e, pair, active)

    @pl.when(inner == 1)
    def _():
        @pl.loop(0, n_tile, unroll=True)
        def _(i):
            second = (
                far_gated[:, columns(i)].astype(jnp.float32) * far_total[:, columns(i)]
            ).astype(jnp.bfloat16)
            far_image[i] = lax.dot_general(
                far_features[...], second, (((0,), (0,)), ((), ())),
                preferred_element_type=jnp.float32,
            ).astype(jnp.bfloat16)
            push(far_image.at[i], image_got.at[i], far_send.at[3], far_recv.at[3], outward)

        @pl.loop(0, subs - EARLY)
        def _(s):
            send_half(n_unit - 1 - EARLY - s, outward, out_send)

    @pl.loop(count - 2 * LAG, count)
    def _(e):
        back(e, pair_of(e), total)

    @pl.when(inner == 0)
    def _():
        @pl.loop(0, EARLY)
        def _(s):
            arrive(n_unit - 1 - s)

        drained(image_got, far_recv.at[3])

    norm0, cross0 = make_image(grad, image0, 0, image_got)
    alpha0 = norm0 / cross0

    @pl.loop(0, n_tile, unroll=True)
    def _(i):
        value = grad[:, columns(i)] - alpha0 * image0[:, columns(i)]
        res_ref[:, columns(i)] = value
        wide = jnp.dot(
            features[...], value.astype(jnp.bfloat16), preferred_element_type=jnp.float32
        )
        active[:, columns(i)] = (gated[:, columns(i)].astype(jnp.float32) * wide).astype(
            jnp.bfloat16
        )
        total[:, columns(i)] = jnp.zeros_like(wide)

    row, col = j_me // 2, j_me % 2
    beside, below = 2 * row + 1 - col, 2 * (1 - row) + col
    across = n_tp - 1 - j_me
    top, low = pl.ds(0, rows // 2), pl.ds(rows // 2, rows // 2)

    def piece_rows(piece, place):
        return pl.ds(pl.multiple_of(piece * rows + place * (rows // 2), 16), rows // 2)

    side, under = {"task": t_me, "tp": beside}, {"task": t_me, "tp": below}
    early = 3 * subs * UNIT // CHUNK

    def stretch(i):
        c = jnp.where(i < early, i, n_chunk - 1 + early - i)
        start = c * CHUNK + upper * (width - CHUNK - 2 * c * CHUNK)
        return c, pl.ds(pl.multiple_of(start, CHUNK), CHUNK)

    def product2(i):
        c, where = stretch(i)

        @pl.when((inner == 0) & (i >= early))
        def _():
            for k in range(CHUNK // UNIT - 1, -1, -1):
                p = CHUNK // UNIT * c + k

                @pl.when(p >= 3 * subs)
                def _(p=p):
                    @pl.when(p < n_unit - EARLY)
                    def _():
                        arrive(p)

                    completed(p)

        partial_sum = lax.dot_general(
            active[...], weights[where, :], (((1,), (1,)), ((), ())),
            preferred_element_type=jnp.float32,
        )
        part2[i] = partial_sum.astype(jnp.bfloat16)
        push(part2.at[i, piece_rows(across, 0)], pass2.at[i, 0], rs_send2.at[0], pass_recv2.at[i], side)
        push(part2.at[i, piece_rows(across, 1)], pass2.at[i, 1], rs_send2.at[0], pass_recv2.at[i], under)
        push(part2.at[i, piece_rows(beside, 0)], got2.at[i, 0, 0], rs_send2.at[0], rs_recv2.at[i], side)
        push(part2.at[i, piece_rows(below, 1)], got2.at[i, 1, 1], rs_send2.at[0], rs_recv2.at[i], under)

    def relay(i):
        drained(pass2.at[i], pass_recv2.at[i])
        for place, piece, target in ((0, below, under), (1, beside, side)):
            added2[i, place] = (
                part2[i, piece_rows(piece, place)].astype(jnp.float32) + pass2[i, place].astype(jnp.float32)
            ).astype(jnp.bfloat16)
            push(
                added2.at[i, place], got2.at[i, 1 - place, place],
                rs_send2.at[0], rs_recv2.at[i], target,
            )

    def reduce2(i):
        drained(got2.at[i], rs_recv2.at[i])
        for place, where in ((0, top), (1, low)):
            mixed2[i, j_me, where] = (
                part2[i, piece_rows(j_me, place)].astype(jnp.float32)
                + got2[i, 0, place].astype(jnp.float32)
                + got2[i, 1, place].astype(jnp.float32)
            ).astype(jnp.bfloat16)
        for target in (side, under):
            push(
                mixed2.at[i, j_me], mixed2.at[i, j_me],
                ag_send2.at[0], ag_recv2.at[i], target,
            )

    def forward2(i):
        drained(mixed2.at[i, pl.ds(0, 2)], ag_recv2.at[i])
        for source, where, target in ((beside, top, under), (below, low, side)):
            piece = mixed2.at[i, source, where]
            push(piece, piece, fw_send.at[0], fw_recv.at[i], target)

    def back2(i):
        _, where = stretch(i)
        drained(mixed2.at[i, 0], fw_recv.at[i])
        total[...] += jnp.dot(
            mixed2[i].reshape(tokens, CHUNK), weights[where, :],
            preferred_element_type=jnp.float32,
        )

    ready = early - (n_chunk - early)

    @pl.loop(0, early)
    def _(i):
        product2(i)

    @pl.loop(0, early)
    def _(i):
        relay(i)

    @pl.loop(0, early)
    def _(i):
        reduce2(i)

    @pl.loop(early, n_chunk)
    def _(i):
        product2(i)

    @pl.loop(early, n_chunk)
    def _(i):
        relay(i)

    @pl.loop(0, early)
    def _(i):
        forward2(i)

    @pl.loop(early, n_chunk)
    def _(i):
        reduce2(i)

    @pl.loop(0, ready)
    def _(i):
        back2(i)

    @pl.loop(early, n_chunk)
    def _(i):
        forward2(i)

    @pl.loop(ready, n_chunk)
    def _(i):
        back2(i)

    norm1, cross1 = make_image(res_ref, image1, 1, None)
    ratio = norm1 / norm0
    alpha1 = norm1 / (cross1 - ratio * norm1 / alpha0)

    @pl.loop(0, n_tile, unroll=True)
    def _(i):
        first, then = grad[:, columns(i)], res_ref[:, columns(i)]
        sol_ref[:, columns(i)] = alpha0 * first + alpha1 * (then + ratio * first)
        res_ref[:, columns(i)] = then - alpha1 * (
            image1[:, columns(i)] + ratio * image0[:, columns(i)]
        )

    drained(weights.at[pl.ds(0, n_unit * HALF)], d2d_send.at[0])

    @pl.when(inner == 0)
    def _():
        drained(weights.at[pl.ds(0, subs * HALF)], in_send.at[0])
        for place, ref in enumerate((features, vector16, gated)):
            drained(ref, far_send.at[place])
        for sem in (rs_send1, ag_send1):
            drained(got1.at[pl.ds(0, short)], sem.at[0])

    @pl.when(inner == 1)
    def _():
        drained(weights.at[pl.ds(0, 2 * subs * HALF)], in_send.at[0])
        drained(weights.at[pl.ds(0, 3 * subs * HALF)], out_send.at[0])
        drained(far_image, far_send.at[3])
        for sem in (rs_send1, ag_send1):
            drained(got1.at[pl.ds(0, slots + n_far)], sem.at[0])

    every = pl.ds(0, n_chunk)
    drained(mixed2.at[every, pl.ds(0, 3)], rs_send2.at[0])
    drained(mixed2.at[every, pl.ds(0, 2)], ag_send2.at[0])
    drained(mixed2.at[every, 0], fw_send.at[0])
    for slot in range(2):
        drained(sums_got.at[slot], sum_send.at[slot])


def settle(first, second, first_out, second_out):
    first_out[...] = first[...]
    second_out[...] = second[...]


def fused(n_tp, support_x, adapter_a, gate_pre, lengths, damping, down_w, grad_b):
    tokens, width = support_x.shape[1:]
    rank = adapter_a.shape[2]
    hidden, share = down_w.shape
    subs = share // HALF
    n_unit = 4 * subs
    middle = arrival_order(subs)[1]
    slots = len(middle) // 2 + sum(1 for pair in far_pairs(middle, subs) if pair)
    rows = tokens // n_tp
    n_chunk = width // CHUNK
    tile = next(size for size in (512, 256, 128) if hidden % size == 0)
    f32, bf16 = jnp.float32, jnp.bfloat16
    dma = pltpu.SemaphoreType.DMA
    anywhere, vmem = pl.BlockSpec(memory_space=pl.ANY), pl.BlockSpec(memory_space=pltpu.VMEM)
    smem = pl.BlockSpec(memory_space=pltpu.SMEM)
    shape = jax.ShapeDtypeStruct((rank, hidden), f32)
    solved, residual = pl.pallas_call(
        kernel,
        out_shape=(shape, shape),
        in_specs=[anywhere, anywhere, anywhere, smem, smem, anywhere, anywhere],
        out_specs=(vmem, vmem),
        scratch_shapes=[
            pltpu.VMEM((rank, width), bf16),
            pltpu.VMEM((rank, hidden), f32),
            pltpu.VMEM((width, hidden), bf16),
            pltpu.VMEM((tokens, hidden), bf16),
            pltpu.VMEM((tokens, hidden), bf16),
            pltpu.VMEM((tokens, hidden), f32),
            pltpu.VMEM((tokens, rank), bf16),
            pltpu.VMEM((rank, hidden), f32),
            pltpu.VMEM((rank, hidden), f32),
            pltpu.VMEM((tokens, hidden), bf16),
            pltpu.VMEM((tokens, hidden), bf16),
            pltpu.VMEM((tokens, hidden), f32),
            pltpu.VMEM((tokens, rank), bf16),
            pltpu.VMEM((rank, hidden), bf16),
            pltpu.VMEM((rank, hidden), bf16),
            pltpu.VMEM((hidden // tile, rank, tile), bf16),
            pltpu.VMEM((hidden // tile, rank, tile), bf16),
            pltpu.VMEM((slots, n_tp, rows, PAIR), bf16),
            pltpu.VMEM((slots, n_tp - 1, rows, PAIR), bf16),
            pltpu.VMEM((slots, n_tp, rows, PAIR), bf16),
            pltpu.VMEM((n_chunk, tokens, CHUNK), bf16),
            pltpu.VMEM((n_chunk, 2, rows // 2, CHUNK), bf16),
            pltpu.VMEM((n_chunk, 2, rows // 2, CHUNK), bf16),
            pltpu.VMEM((n_chunk, 2, 2, rows // 2, CHUNK), bf16),
            pltpu.VMEM((n_chunk, n_tp, rows, CHUNK), bf16),
            pltpu.VMEM((2, 2, 8, 128), f32),
            pltpu.VMEM((2, n_tp - 1, 2, 8, 128), f32),
            dma((5,)),
            dma((n_unit,)),
            dma((n_unit,)),
            dma((1,)),
            dma((1,)),
            dma((1,)),
            dma((4,)),
            dma((4,)),
            dma((1,)),
            dma((slots,)),
            dma((1,)),
            dma((slots,)),
            dma((1,)),
            dma((n_chunk,)),
            dma((n_chunk,)),
            dma((1,)),
            dma((n_chunk,)),
            dma((1,)),
            dma((n_chunk,)),
            dma((2,)),
            dma((2,)),
        ],
        compiler_params=pltpu.CompilerParams(
            collective_id=0, has_side_effects=True, vmem_limit_bytes=66_000_000
        ),
    )(
        support_x[0], adapter_a[0].T, gate_pre[0], lengths, damping, down_w.T, grad_b[0]
    )
    solved, residual = pl.pallas_call(
        settle,
        out_shape=(shape, shape),
        in_specs=[vmem, vmem],
        out_specs=(vmem, vmem),
    )(solved, residual)
    return solved[None], residual[None]


def solution(mesh):
    in_specs = (
        P("task", None, None),
        P("task", None, None),
        P("task", None, "tp"),
        P("task"),
        P("task"),
        P("tp", "task"),
        P("task", None, "tp"),
    )
    out_specs = (P("task", None, "tp"), P("task", None, "tp"))
    n_task, n_tp = mesh.shape["task"], mesh.shape["tp"]

    def body(support_x, *rest):
        tokens, width = support_x.shape[1:]
        hidden, share = rest[4].shape
        even = tokens % (32 * n_tp) == 0 and hidden % 128 == 0
        if n_tp != 4 or n_task != 8 or share % HALF or width % CHUNK or not even:
            return shards(support_x, *rest)
        return fused(n_tp, support_x, *rest)

    return jax.shard_map(body, mesh=mesh, in_specs=in_specs, out_specs=out_specs, check_vma=False)
```
